32 devices in a mesh: slab: 8 (over z, y), layer: 4 (over x, core).
Axes of the slice: x: 2, y: 2, z: 4, core: 2. Of those that a mesh axis runs over, the one named last changes fastest.
Arguments:
- hamilton_blocks: bfloat16 [128, 128, 128], P(('slab', 'layer')), may hold values from -0.25 to 0.25
- pair_ids: int32 [32, 10], P(('slab', 'layer')), may hold values from 0 to 127, as said below
- weights: float32 [32, 10], P(('slab', 'layer')), may hold values from 0.25 to 4
- potential: float32 [1], replicated, may hold values from -1 to 1
Outputs:
- density: float32 [128, 128, 128], P(('slab', 'layer'))
- energy: float32 [128, 128, 128], P(('slab', 'layer'))
The draws below stay inside these ranges and needn't reach their ends.
Inputs may be any that keep to these rules, and one draw needn't show every extreme that they name: `pair_ids`: the entries of one row are distinct. Slot p is owned by device p // 4, whose slab index is that device // 4 and layer index that device % 4. Row d names only slots owned by devices whose slab index is that of device d, or one more or one less cyclically over 8, with any layer index. A row names at most 4 slots of any one device, and exactly 4 of some device; in every draw some device has exactly 4 of its slots named by each of the 3 * 4 rows that may name its slots.
All inputs are finite; a program needn't handle non-finite values.
Results may differ from the reference program's by a relative error of at most 0.0017.
Values may be sent and summed in bfloat16 or wider, within the bound.
No kernel may reach another device: no remote copies, remote signals or barrier semaphores. Data moves between devices by JAX's collectives and lax.ppermute only.
A program may use at most 64 MiB of HBM per device.

```python
import math
import jax
import jax.numpy as jnp
import numpy as np
from jax import lax

BS = 128
NB = 4
PAIRS_DEV = 4
CAP = 4
ITERS = 2
NPS = 10
ORDER = 512
NPAIRS = 128
N_SLAB = 8
N_LAYER = 4
DEVICES = 32


def draw_pair_ids(key, part):
    owners = 3 * N_LAYER
    base = jax.random.fold_in(key, 17)
    shift_key = jax.random.fold_in(base, 1)
    layer_key = jax.random.fold_in(base, 2)
    pool_key = jax.random.fold_in(base, 3)
    slot_key = jax.random.fold_in(base, 4)
    order_key = jax.random.fold_in(base, 5)
    residue = jax.random.randint(shift_key, (), 0, 3)
    hub_layers = jax.random.randint(layer_key, (N_SLAB,), 0, N_LAYER)
    device = jnp.arange(DEVICES, dtype=jnp.int32)
    here_slab = device // N_LAYER
    offsets = jnp.arange(3, dtype=jnp.int32)
    near_slab = (here_slab[:, None] + offsets[None, :] - 1 + N_SLAB) % N_SLAB
    marked = near_slab % 3 == residue
    first_mark = jnp.min(jnp.where(marked, offsets[None, :], 3), axis=1)
    hub_offset = jnp.where(first_mark == 3, 1, first_mark)
    hub_slab = (here_slab + hub_offset - 1 + N_SLAB) % N_SLAB
    hub_local = (hub_offset * N_LAYER + hub_layers[hub_slab]).astype(jnp.int32)
    pool_base = jnp.repeat(jnp.arange(owners - 1, dtype=jnp.int32), CAP)

    def pick_rest(subkey):
        return jax.random.permutation(subkey, pool_base)[:NPS - CAP]
    rest = jax.vmap(pick_rest)(jax.random.split(pool_key, DEVICES)).astype(jnp.int32)
    rest = rest + (rest >= hub_local[:, None]).astype(jnp.int32)
    labels = jnp.concatenate([jnp.broadcast_to(hub_local[:, None], (DEVICES, CAP)), rest], axis=1)
    items = jnp.arange(NPS, dtype=jnp.int32)
    same = labels[:, :, None] == labels[:, None, :]
    earlier = items[None, :] < items[:, None]
    ranks = jnp.sum(jnp.logical_and(same, earlier[None]), axis=2).astype(jnp.int32)

    def slot_order(subkey):
        return jax.random.permutation(subkey, PAIRS_DEV)
    slot_perms = jax.vmap(slot_order)(jax.random.split(slot_key, DEVICES * owners)).astype(jnp.int32)
    slot_perms = slot_perms.reshape(DEVICES, owners, PAIRS_DEV)
    slots = slot_perms[device[:, None], labels, ranks]

    def item_order(subkey):
        return jax.random.permutation(subkey, NPS)
    orders = jax.vmap(item_order)(jax.random.split(order_key, DEVICES)).astype(jnp.int32)
    labels = jnp.take_along_axis(labels, orders, axis=1)
    slots = jnp.take_along_axis(slots, orders, axis=1)
    owner_slab = (here_slab[:, None] + labels // N_LAYER - 1 + N_SLAB) % N_SLAB
    owner_layer = labels % N_LAYER
    return ((owner_slab * N_LAYER + owner_layer) * PAIRS_DEV + slots).astype(jnp.int32)


def shard_levels(stream_key, extent, pieces, smallest, top_value):
    level = 1.0
    for dim, blocks in pieces:
        heights = jax.random.uniform(jax.random.fold_in(jax.random.fold_in(stream_key, 6), dim), (blocks,), jnp.float32, smallest / len(pieces), top_value / len(pieces))
        level = level * jnp.repeat(jnp.exp(heights), extent[dim] // blocks).reshape((-1,) + (1,) * (len(extent) - 1 - dim))
    return level


def noise(key, shape, scale, reach, cuts=(), held_as=jnp.bfloat16):
    values = jax.random.normal(key, shape, jnp.float32) * scale
    if len(cuts) > 0:
        values = shard_levels(key, shape, cuts, -0.22, 0.18) * values
    return jnp.clip(values, min=-reach, max=reach).astype(held_as)


def setup_inputs(seed: int = 0) -> dict:
    keys = jax.random.split(jax.random.key(seed), 5)
    return {
        "hamilton_blocks": noise(keys[0], (NPAIRS, BS, BS), ORDER ** -0.5, 0.25, ((0, 32),)),
        "pair_ids": draw_pair_ids(jax.random.fold_in(keys[4], 71), 0),
        "weights": jnp.clip(jnp.exp(math.log(4.0) - 2.7725887 * jax.random.uniform(keys[2], (DEVICES, NPS), jnp.float32) ** shard_levels(keys[2], (DEVICES, NPS), ((0, 32),), -0.2, 0.2)), 0.25, 4.0),
        "potential": jnp.clip(jax.random.uniform(keys[3], (1,), jnp.float32, -1.0, 1.0), -1.0, 1.0),
    }


def submatrix_step(blocks, weight_row, mu_value):
    block_rows, block_cols = np.triu_indices(NB)
    block_rows = block_rows.astype(np.int32)
    block_cols = block_cols.astype(np.int32)
    upper_grid = jnp.zeros((NB, NB, BS, BS), jnp.float32).at[block_rows, block_cols].set(blocks.astype(jnp.float32))
    sub_order = NB * BS
    upper = upper_grid.transpose(0, 2, 1, 3).reshape(sub_order, sub_order)
    hamilt = upper + upper.T
    identity = jnp.eye(sub_order, dtype=jnp.float32)
    shifted = mu_value * identity - hamilt
    norm_scale = 2.0 * jnp.sqrt(jnp.sum(shifted * shifted) / sub_order + 1e-06)
    iterate = shifted / norm_scale
    for iteration in range(ITERS):
        square = jnp.dot(iterate, iterate, precision=lax.Precision.HIGHEST, preferred_element_type=jnp.float32)
        iterate = 1.5 * iterate - 0.5 * jnp.dot(iterate, square, precision=lax.Precision.HIGHEST, preferred_element_type=jnp.float32)
    dens_sub = 0.5 * (identity + iterate)
    energy_sub = jnp.dot(dens_sub, hamilt, precision=lax.Precision.HIGHEST, preferred_element_type=jnp.float32)
    dens_pairs = dens_sub.reshape(NB, BS, NB, BS).transpose(0, 2, 1, 3)[block_rows, block_cols]
    energy_pairs = energy_sub.reshape(NB, BS, NB, BS).transpose(0, 2, 1, 3)[block_rows, block_cols]
    scaled = weight_row[:, None, None]
    return ((scaled * dens_pairs).astype(jnp.bfloat16), (scaled * energy_pairs).astype(jnp.bfloat16))

def reference(hamilton_blocks, pair_ids, weights, potential):

    def one_device(totals, device):
        requests = pair_ids[device].astype(jnp.int32)
        blocks = hamilton_blocks[requests]
        dens_parts, energy_parts = submatrix_step(blocks, weights[device], potential[0])
        dens_total = totals[0].at[requests].add(dens_parts.astype(jnp.float32))
        energy_total = totals[1].at[requests].add(energy_parts.astype(jnp.float32))
        return ((dens_total, energy_total), None)
    empty = jnp.zeros((NPAIRS, BS, BS), jnp.float32)
    totals, unused = lax.scan(one_device, (empty, empty), jnp.arange(DEVICES, dtype=jnp.int32))
    return (totals[0], totals[1])
```

```python
import functools

import jax
import jax.numpy as jnp
import numpy as np
from jax import lax
from jax.experimental import pallas as pl
from jax.experimental.pallas import tpu as pltpu
from jax.sharding import PartitionSpec as P

ITERS = 2
AXES = ("slab", "layer")


def block_order(pair_count):
    return (int(np.sqrt(8 * pair_count + 1)) - 1) // 2


def halves(value):
    high = value.astype(jnp.bfloat16)
    low = (value - high.astype(jnp.float32)).astype(jnp.bfloat16)
    return high, low


def mm(left, right):
    return jnp.dot(left, right, preferred_element_type=jnp.float32)


def step_kernel(
    sizes, place, ids, weights, potential, near, far, kept, sent,
    shift_hi, shift_lo, ham_hi, ham_lo, a_hi, a_lo, b_hi, b_lo, full, full2, kept_sum, sent_sum,
):
    slabs, groups, cores, pieces, rows, nb, bs = sizes
    order = nb * bs
    wide = min(2 * bs, order)
    half_count = order // wide
    f32, bf16 = jnp.float32, jnp.bfloat16
    here_slab, here_group, here_core = place[0], place[1], place[2]
    mu = potential[0]
    eye_block = (
        lax.broadcasted_iota(jnp.int32, (bs, bs), 0) == lax.broadcasted_iota(jnp.int32, (bs, bs), 1)
    )
    eye = (
        lax.broadcasted_iota(jnp.int32, (order, order), 0)
        == lax.broadcasted_iota(jnp.int32, (order, order), 1)
    )
    kept_sum[...] = jnp.zeros_like(kept_sum)
    if cores > 1:
        sent_sum[...] = jnp.zeros_like(sent_sum)
    shift_lo[...] = jnp.zeros_like(shift_lo)
    ham_lo[...] = jnp.zeros_like(ham_lo)
    pairs = [(a, b) for a in range(nb) for b in range(a, nb)]

    def where_is(row, k):
        slot_id = ids[row, k]
        slot = slot_id % pieces
        device = slot_id // pieces
        layer = device % (groups * cores)
        offset = (device // (groups * cores) - here_slab + 1 + slabs) % slabs
        return offset, layer // cores, layer % cores, slot

    def cut(index):
        return pl.ds(index * bs, bs)

    def low_cut(index):
        part = index * bs % wide
        return index * bs // wide, pl.ds(part, bs), pl.ds(part, bs)

    for row in range(rows):
        squares = jnp.zeros((bs, bs), f32)
        for k, (a, b) in enumerate(pairs):
            offset, group, core, slot = where_is(row, k)
            turn = (here_group - group + groups) % groups
            index = (turn * 3 + offset) * pieces + slot
            block = near[index]
            if cores > 1:
                block = jnp.where(core == here_core, block, far[index])
            block = block.astype(f32)
            flipped = block.T
            if a == b:
                ham = block + flipped
                shift = jnp.where(eye_block, mu, 0.0) - ham
                squares += shift * shift
                high, low = halves(shift)
                shift_hi[cut(a), cut(a)] = high
                shift_lo[low_cut(a)] = low
                high, low = halves(ham)
                ham_hi[cut(a), cut(a)] = high
                ham_lo[low_cut(a)] = low
            else:
                squares += 2.0 * (block * block)
                ham_hi[cut(a), cut(b)] = block.astype(bf16)
                ham_hi[cut(b), cut(a)] = flipped.astype(bf16)
                shift_hi[cut(a), cut(b)] = (-block).astype(bf16)
                shift_hi[cut(b), cut(a)] = (-flipped).astype(bf16)
        total = jnp.sum(squares, axis=(0, 1), keepdims=True)
        inverse = 1.0 / (2.0 * jnp.sqrt(total / order + 1e-06))

        full[...] = mm(shift_hi[...], shift_hi[...])
        for j in range(half_count):
            part = pl.ds(j * wide, wide)
            full[:, part] += mm(shift_hi[:, part], shift_lo[j])
            full[part, :] += mm(shift_lo[j], shift_hi[part, :])
        factor = jnp.where(eye, 1.5, 0.0) - (0.5 * inverse * inverse) * full[...]
        b_hi[...], b_lo[...] = halves(factor)
        full[...] = mm(shift_hi[...], b_hi[...]) + mm(shift_hi[...], b_lo[...])
        for j in range(half_count):
            part = pl.ds(j * wide, wide)
            full[part, :] += mm(shift_lo[j], b_hi[part, :])
        a_hi[...], a_lo[...] = halves(inverse * full[...])
        for _ in range(ITERS - 1):
            full[...] = mm(a_hi[...], a_hi[...]) + mm(a_hi[...], a_lo[...]) + mm(a_lo[...], a_hi[...])
            factor = jnp.where(eye, 1.5, 0.0) - 0.5 * full[...]
            b_hi[...], b_lo[...] = halves(factor)
            full[...] = mm(a_hi[...], b_hi[...]) + mm(a_hi[...], b_lo[...]) + mm(a_lo[...], b_hi[...])
            if _ < ITERS - 2:
                a_hi[...], a_lo[...] = halves(full[...])
        dens = 0.5 * (jnp.where(eye, 1.0, 0.0) + full[...])
        full[...] = dens
        a_hi[...], a_lo[...] = halves(dens)
        for i in range(half_count):
            upper = pl.ds(i * wide, wide)
            right = pl.ds(i * wide, order - i * wide)
            full2[upper, right] = mm(a_hi[upper, :], ham_hi[:, right]) + mm(a_lo[upper, :], ham_hi[:, right])
            for j in range(i, half_count):
                part = pl.ds(j * wide, wide)
                full2[upper, part] += mm(a_hi[upper, part], ham_lo[j])
        for k, (a, b) in enumerate(pairs):
            offset, group, core, slot = where_is(row, k)
            weight = weights[row, k]

            def add(target):
                at = offset * pieces + slot
                for mat, source in ((0, full), (1, full2)):
                    part = (weight * source[cut(a), cut(b)]).astype(bf16).astype(f32)
                    target[mat, at] += part

            @pl.when(jnp.logical_and(group == here_group, core == here_core))
            def _():
                add(kept_sum)

            if cores > 1:

                @pl.when(jnp.logical_and(group == here_group, core != here_core))
                def _():
                    add(sent_sum)

    kept[...] = kept_sum[...]
    if cores > 1:
        sent[...] = sent_sum[...].astype(bf16)


def shards(hamilton_blocks, pair_ids, weights, potential):
    pieces, bs, _ = hamilton_blocks.shape
    slabs = lax.axis_size("slab")
    layers = lax.axis_size("layer")
    cores = 2 if layers % 2 == 0 else 1
    groups = layers // cores
    pair_count = pair_ids.shape[1]
    nb = block_order(pair_count)
    order = nb * bs
    wide = min(2 * bs, order)

    def send(value, slab_step, group_step, core_step):
        pairs = []
        for s in range(slabs):
            for g in range(groups):
                for c in range(cores):
                    there = ((s + slab_step) % slabs * groups + (g + group_step) % groups) * cores
                    pairs.append(((s * groups + g) * cores + c, there + (c + core_step) % cores))
        return lax.ppermute(value, AXES, pairs)

    table = []
    for g in range(groups):
        for s in (1, 0, -1):
            table.append(hamilton_blocks if (s, g) == (0, 0) else send(hamilton_blocks, s, g, 0))
    ids = jnp.concatenate([pair_ids] + [send(pair_ids, 0, g, 0) for g in range(1, groups)])
    scales = jnp.concatenate([weights] + [send(weights, 0, g, 0) for g in range(1, groups)])
    near = jnp.concatenate(table)
    far = send(near, 0, 0, 1) if cores > 1 else near
    here_layer = lax.axis_index("layer")
    place = jnp.stack([lax.axis_index("slab"), here_layer // cores, here_layer % cores]).astype(jnp.int32)

    sizes = (slabs, groups, cores, pieces, groups, nb, bs)
    smem = pl.BlockSpec(memory_space=pltpu.SMEM)
    vmem = pl.BlockSpec(memory_space=pltpu.VMEM)
    f32, bf16 = jnp.float32, jnp.bfloat16
    square = lambda dtype: pltpu.VMEM((order, order), dtype)
    slots = 3 * pieces
    kept, sent = pl.pallas_call(
        functools.partial(step_kernel, sizes),
        out_shape=(
            jax.ShapeDtypeStruct((2, slots, bs, bs), f32),
            jax.ShapeDtypeStruct((2, slots, bs, bs), bf16),
        ),
        in_specs=[smem, smem, smem, smem, vmem, vmem],
        out_specs=(vmem, vmem),
        scratch_shapes=[
            square(bf16),
            pltpu.VMEM((order // wide, wide, wide), bf16),
            square(bf16),
            pltpu.VMEM((order // wide, wide, wide), bf16),
            square(bf16), square(bf16), square(bf16), square(bf16),
            square(f32), square(f32),
            pltpu.VMEM((2, slots, bs, bs), f32),
            pltpu.VMEM((2, slots, bs, bs), f32),
        ],
        name="submatrix_step",
    )(place, ids, scales, potential, near, far)
    if cores > 1:
        kept = kept + send(sent, 0, 0, 1).astype(f32)
    kept = kept.reshape(2, 3, pieces, bs, bs)
    back = send(kept[:, 0].astype(bf16), -1, 0, 0)
    ahead = send(kept[:, 2].astype(bf16), 1, 0, 0)
    totals = kept[:, 1] + back.astype(f32) + ahead.astype(f32)
    return totals[0], totals[1]


def solution(mesh):
    placed = (P(AXES, None, None), P(AXES, None), P(AXES, None), P())
    return jax.shard_map(
        shards,
        mesh=mesh,
        in_specs=placed,
        out_specs=(P(AXES, None, None), P(AXES, None, None)),
        check_vma=False,
    )
```

```python
import functools

import jax
import jax.numpy as jnp
import numpy as np
from jax import lax
from jax.experimental import pallas as pl
from jax.experimental.pallas import tpu as pltpu
from jax.sharding import PartitionSpec as P

ITERS = 2
AXES = ("slab", "layer")


def block_order(pair_count):
    return (int(np.sqrt(8 * pair_count + 1)) - 1) // 2


def halves(value):
    high = value.astype(jnp.bfloat16)
    low = (value - high.astype(jnp.float32)).astype(jnp.bfloat16)
    return high, low


def mm(left, right):
    return jnp.dot(left, right, preferred_element_type=jnp.float32)


def step_kernel(
    sizes, *refs
):
    slabs, groups, cores, pieces, rows, nb, bs = sizes
    ids, weights = refs[:rows], refs[rows : 2 * rows]
    (
        potential, near, far, kept_back, kept_here, kept_ahead, sent,
        shift_hi, shift_lo, ham_hi, ham_lo, a_hi, a_lo, b_hi, b_lo, full, full2, kept_sum, sent_sum,
    ) = refs[2 * rows :]
    order = nb * bs
    wide = min(2 * bs, order)
    half_count = order // wide
    f32, bf16 = jnp.float32, jnp.bfloat16
    here_slab = lax.axis_index("slab")
    here_layer = lax.axis_index("layer")
    here_group, here_core = here_layer // cores, here_layer % cores
    mu = potential[0]
    eye_block = (
        lax.broadcasted_iota(jnp.int32, (bs, bs), 0) == lax.broadcasted_iota(jnp.int32, (bs, bs), 1)
    )
    eye = (
        lax.broadcasted_iota(jnp.int32, (order, order), 0)
        == lax.broadcasted_iota(jnp.int32, (order, order), 1)
    )
    kept_sum[...] = jnp.zeros_like(kept_sum)
    if cores > 1:
        sent_sum[...] = jnp.zeros_like(sent_sum)
    shift_lo[...] = jnp.zeros_like(shift_lo)
    ham_lo[...] = jnp.zeros_like(ham_lo)
    pairs = [(a, b) for a in range(nb) for b in range(a, nb)]

    def where_is(row, k):
        slot_id = ids[row][0, k]
        slot = slot_id % pieces
        device = slot_id // pieces
        layer = device % (groups * cores)
        offset = (device // (groups * cores) - here_slab + 1 + slabs) % slabs
        return offset, layer // cores, layer % cores, slot

    def cut(index):
        return pl.ds(index * bs, bs)

    def low_cut(index):
        part = index * bs % wide
        return index * bs // wide, pl.ds(part, bs), pl.ds(part, bs)

    for row in range(rows):
        squares = jnp.zeros((bs, bs), f32)
        for k, (a, b) in enumerate(pairs):
            offset, group, core, slot = where_is(row, k)
            turn = (here_group - group + groups) % groups
            index = (turn * 3 + offset) * pieces + slot
            block = near[index]
            if cores > 1:
                block = jnp.where(core == here_core, block, far[index])
            block = block.astype(f32)
            flipped = block.T
            if a == b:
                ham = block + flipped
                shift = jnp.where(eye_block, mu, 0.0) - ham
                squares += shift * shift
                high, low = halves(shift)
                shift_hi[cut(a), cut(a)] = high
                shift_lo[low_cut(a)] = low
                high, low = halves(ham)
                ham_hi[cut(a), cut(a)] = high
                ham_lo[low_cut(a)] = low
            else:
                squares += 2.0 * (block * block)
                ham_hi[cut(a), cut(b)] = block.astype(bf16)
                ham_hi[cut(b), cut(a)] = flipped.astype(bf16)
                shift_hi[cut(a), cut(b)] = (-block).astype(bf16)
                shift_hi[cut(b), cut(a)] = (-flipped).astype(bf16)
        total = jnp.sum(squares, axis=(0, 1), keepdims=True)
        inverse = 1.0 / (2.0 * jnp.sqrt(total / order + 1e-06))

        full[...] = mm(shift_hi[...], shift_hi[...])
        for j in range(half_count):
            part = pl.ds(j * wide, wide)
            full[:, part] += mm(shift_hi[:, part], shift_lo[j])
            full[part, :] += mm(shift_lo[j], shift_hi[part, :])
        factor = jnp.where(eye, 1.5, 0.0) - (0.5 * inverse * inverse) * full[...]
        b_hi[...], b_lo[...] = halves(factor)
        full[...] = mm(shift_hi[...], b_hi[...]) + mm(shift_hi[...], b_lo[...])
        for j in range(half_count):
            part = pl.ds(j * wide, wide)
            full[part, :] += mm(shift_lo[j], b_hi[part, :])
        a_hi[...], a_lo[...] = halves(inverse * full[...])
        for _ in range(ITERS - 1):
            full[...] = mm(a_hi[...], a_hi[...]) + mm(a_hi[...], a_lo[...]) + mm(a_lo[...], a_hi[...])
            factor = jnp.where(eye, 1.5, 0.0) - 0.5 * full[...]
            b_hi[...], b_lo[...] = halves(factor)
            full[...] = mm(a_hi[...], b_hi[...]) + mm(a_hi[...], b_lo[...]) + mm(a_lo[...], b_hi[...])
            if _ < ITERS - 2:
                a_hi[...], a_lo[...] = halves(full[...])
        dens = 0.5 * (jnp.where(eye, 1.0, 0.0) + full[...])
        full[...] = dens
        a_hi[...], a_lo[...] = halves(dens)
        for i in range(half_count):
            upper = pl.ds(i * wide, wide)
            right = pl.ds(i * wide, order - i * wide)
            full2[upper, right] = mm(a_hi[upper, :], ham_hi[:, right]) + mm(a_lo[upper, :], ham_hi[:, right])
            for j in range(i, half_count):
                part = pl.ds(j * wide, wide)
                full2[upper, part] += mm(a_hi[upper, part], ham_lo[j])
        for k, (a, b) in enumerate(pairs):
            offset, group, core, slot = where_is(row, k)
            weight = weights[row][0, k]

            def add(target):
                at = offset * pieces + slot
                for mat, source in ((0, full), (1, full2)):
                    part = (weight * source[cut(a), cut(b)]).astype(bf16).astype(f32)
                    target[mat, at] += part

            @pl.when(jnp.logical_and(group == here_group, core == here_core))
            def _():
                add(kept_sum)

            if cores > 1:

                @pl.when(jnp.logical_and(group == here_group, core != here_core))
                def _():
                    add(sent_sum)

    for offset, kept in enumerate((kept_back, kept_here, kept_ahead)):
        kept[...] = kept_sum[:, pl.ds(offset * pieces, pieces)]
    if cores > 1:
        sent[...] = sent_sum[...].astype(bf16)


def shards(hamilton_blocks, pair_ids, weights, potential):
    pieces, bs, _ = hamilton_blocks.shape
    slabs = lax.axis_size("slab")
    layers = lax.axis_size("layer")
    cores = 2 if layers % 2 == 0 else 1
    groups = layers // cores
    pair_count = pair_ids.shape[1]
    nb = block_order(pair_count)
    order = nb * bs
    wide = min(2 * bs, order)

    def send(value, slab_step, group_step, core_step):
        pairs = []
        for s in range(slabs):
            for g in range(groups):
                for c in range(cores):
                    there = ((s + slab_step) % slabs * groups + (g + group_step) % groups) * cores
                    pairs.append(((s * groups + g) * cores + c, there + (c + core_step) % cores))
        return lax.ppermute(value, AXES, pairs)

    table = []
    for g in range(groups):
        for s in (1, 0, -1):
            table.append(hamilton_blocks if (s, g) == (0, 0) else send(hamilton_blocks, s, g, 0))
    ids = [pair_ids] + [send(pair_ids, 0, g, 0) for g in range(1, groups)]
    scales = [weights] + [send(weights, 0, g, 0) for g in range(1, groups)]
    near, ids, scales = lax.optimization_barrier((jnp.concatenate(table), ids, scales))
    far = send(near, 0, 0, 1) if cores > 1 else near
    sizes = (slabs, groups, cores, pieces, groups, nb, bs)
    smem = pl.BlockSpec(memory_space=pltpu.SMEM)
    vmem = pl.BlockSpec(memory_space=pltpu.VMEM)
    f32, bf16 = jnp.float32, jnp.bfloat16
    square = lambda dtype: pltpu.VMEM((order, order), dtype)
    slots = 3 * pieces
    *kept, sent = pl.pallas_call(
        functools.partial(step_kernel, sizes),
        out_shape=[jax.ShapeDtypeStruct((2, pieces, bs, bs), f32)] * 3
        + [jax.ShapeDtypeStruct((2, slots, bs, bs), bf16)],
        in_specs=[smem] * (2 * groups + 1) + [vmem, vmem],
        out_specs=[vmem] * 4,
        scratch_shapes=[
            square(bf16),
            pltpu.VMEM((order // wide, wide, wide), bf16),
            square(bf16),
            pltpu.VMEM((order // wide, wide, wide), bf16),
            square(bf16), square(bf16), square(bf16), square(bf16),
            square(f32), square(f32),
            pltpu.VMEM((2, slots, bs, bs), f32),
            pltpu.VMEM((2, slots, bs, bs), f32),
        ],
        compiler_params=pltpu.CompilerParams(vmem_limit_bytes=24 * 2**20),
        name="submatrix_step",
    )(*ids, *scales, potential, near, far)
    if cores > 1:
        other = send(sent, 0, 0, 1)
        kept = [
            part + other[:, i * pieces : (i + 1) * pieces].astype(f32) for i, part in enumerate(kept)
        ]
    below = send(kept[0].astype(bf16), -1, 0, 0)
    above = send(kept[2].astype(bf16), 1, 0, 0)
    totals = kept[1] + below.astype(f32) + above.astype(f32)
    return totals[0], totals[1]


def solution(mesh):
    placed = (P(AXES, None, None), P(AXES, None), P(AXES, None), P())
    return jax.shard_map(
        shards,
        mesh=mesh,
        in_specs=placed,
        out_specs=(P(AXES, None, None), P(AXES, None, None)),
        check_vma=False,
    )
```

```python
import functools

import jax
import jax.numpy as jnp
import numpy as np
from jax import lax
from jax.experimental import pallas as pl
from jax.experimental.pallas import tpu as pltpu
from jax.sharding import PartitionSpec as P

ITERS = 2
AXES = ("slab", "layer")


def block_order(pair_count):
    return (int(np.sqrt(8 * pair_count + 1)) - 1) // 2


def halves(value):
    high = value.astype(jnp.bfloat16)
    low = (value - high.astype(jnp.float32)).astype(jnp.bfloat16)
    return high, low


def mm(left, right):
    return jnp.dot(left, right, preferred_element_type=jnp.float32)


def step_kernel(sizes, *refs):
    slabs, groups, cores, pieces, rows, nb, bs = sizes
    ids, weights = refs[:rows], refs[rows : 2 * rows]
    potential, near, far, kept_back, kept_here, kept_ahead, sent = refs[2 * rows : 2 * rows + 7]
    scratch = refs[2 * rows + 7 :]
    per_row = len(scratch) // rows
    order = nb * bs
    wide = min(2 * bs, order)
    half_count = order // wide
    f32, bf16 = jnp.float32, jnp.bfloat16
    here_slab = lax.axis_index("slab")
    here_layer = lax.axis_index("layer")
    here_group, here_core = here_layer // cores, here_layer % cores
    mu = potential[0]
    pairs = [(a, b) for a in range(nb) for b in range(a, nb)]

    def eye(size, value):
        down = lax.broadcasted_iota(jnp.int32, (size, size), 0)
        return jnp.where(down == lax.broadcasted_iota(jnp.int32, (size, size), 1), value, 0.0)

    def where_is(row, k):
        slot_id = ids[row][0, k]
        slot = slot_id % pieces
        device = slot_id // pieces
        layer = device % (groups * cores)
        offset = (device // (groups * cores) - here_slab + 1 + slabs) % slabs
        return offset, layer // cores, layer % cores, slot

    def cut(index):
        return pl.ds(index * bs, bs)

    def low_cut(index):
        part = index * bs % wide
        return index * bs // wide, pl.ds(part, bs), pl.ds(part, bs)

    spots = [[where_is(row, k) for k in range(len(pairs))] for row in range(rows)]
    state = [scratch[row * per_row : (row + 1) * per_row] for row in range(rows)]
    inverses = []

    for row in range(rows):
        base_hi, base_lo, diag_hi, diag_lo = state[row][:4]
        base_lo[...] = jnp.zeros_like(base_lo)
        squares = jnp.zeros((bs, bs), f32)
        for k, (a, b) in enumerate(pairs):
            offset, group, core, slot = spots[row][k]
            turn = (here_group - group + groups) % groups
            index = (turn * 3 + offset) * pieces + slot
            block = near[index]
            if cores > 1:
                block = jnp.where(core == here_core, block, far[index])
            wide_block = block.astype(f32)
            if a == b:
                ham = wide_block + wide_block.T
                base = ham - eye(bs, mu)
                squares += base * base
                base_hi[cut(a), cut(a)], base_lo[low_cut(a)] = halves(base)
                diag_hi[a], diag_lo[a] = halves(ham)
            else:
                squares += 2.0 * (wide_block * wide_block)
                base_hi[cut(a), cut(b)] = block
                base_hi[cut(b), cut(a)] = block.T
        total = jnp.sum(squares, axis=(0, 1), keepdims=True)
        inverses.append(1.0 / (2.0 * jnp.sqrt(total / order + 1e-06)))

    kept = (kept_back, kept_here, kept_ahead)
    for target in kept:
        target[...] = jnp.zeros_like(target)
    if cores > 1:
        sent[...] = jnp.zeros_like(sent)

    for row in range(rows):
        base_hi, base_lo, _, _, _, _, b_hi, b_lo, full, _ = state[row]
        full[...] = mm(base_hi[...], base_hi[...])
        for j in range(half_count):
            part = pl.ds(j * wide, wide)
            full[:, part] += mm(base_hi[:, part], base_lo[j])
            full[part, :] += mm(base_lo[j], base_hi[part, :])
        scale = 0.5 * inverses[row] * inverses[row]
        b_hi[...], b_lo[...] = halves(eye(order, 1.5) - scale * full[...])
    for row in range(rows):
        base_hi, base_lo, diag_hi, diag_lo, a_hi, a_lo, b_hi, b_lo, full, _ = state[row]
        full[...] = mm(base_hi[...], b_hi[...]) + mm(base_hi[...], b_lo[...])
        for j in range(half_count):
            part = pl.ds(j * wide, wide)
            full[part, :] += mm(base_lo[j], b_hi[part, :])
        a_hi[...], a_lo[...] = halves(-inverses[row] * full[...])
        for a in range(nb):
            base_hi[cut(a), cut(a)] = diag_hi[a]
            base_lo[low_cut(a)] = diag_lo[a]
    for step in range(1, ITERS):
        for row in range(rows):
            _, _, _, _, a_hi, a_lo, b_hi, b_lo, full, _ = state[row]
            full[...] = mm(a_hi[...], a_hi[...]) + mm(a_hi[...], a_lo[...]) + mm(a_lo[...], a_hi[...])
            b_hi[...], b_lo[...] = halves(eye(order, 1.5) - 0.5 * full[...])
        for row in range(rows):
            _, _, _, _, a_hi, a_lo, b_hi, b_lo, full, _ = state[row]
            full[...] = mm(a_hi[...], b_hi[...]) + mm(a_hi[...], b_lo[...]) + mm(a_lo[...], b_hi[...])
            if step < ITERS - 1:
                a_hi[...], a_lo[...] = halves(full[...])
    for row in range(rows):
        base_hi, base_lo, _, _, a_hi, a_lo, _, _, full, full2 = state[row]
        dens = 0.5 * (eye(order, 1.0) + full[...])
        full[...] = dens
        a_hi[...], a_lo[...] = halves(dens)
        for i in range(half_count):
            upper = pl.ds(i * wide, wide)
            right = pl.ds(i * wide, order - i * wide)
            full2[upper, right] = mm(a_hi[upper, :], base_hi[:, right]) + mm(a_lo[upper, :], base_hi[:, right])
            for j in range(i, half_count):
                part = pl.ds(j * wide, wide)
                full2[upper, part] += mm(a_hi[upper, part], base_lo[j])
    for row in range(rows):
        full, full2 = state[row][8:]
        for k, (a, b) in enumerate(pairs):
            offset, group, core, slot = spots[row][k]
            weight = weights[row][0, k]

            def add(target, at):
                for mat, source in ((0, full), (1, full2)):
                    part = (weight * source[cut(a), cut(b)]).astype(bf16).astype(f32)
                    target[mat, at] = (target[mat, at].astype(f32) + part).astype(target.dtype)

            mine = jnp.logical_and(group == here_group, core == here_core)
            for place, target in enumerate(kept):

                @pl.when(jnp.logical_and(mine, offset == place))
                def _():
                    add(target, slot)

            if cores > 1:

                @pl.when(jnp.logical_and(group == here_group, core != here_core))
                def _():
                    add(sent, offset * pieces + slot)


def shards(hamilton_blocks, pair_ids, weights, potential):
    pieces, bs, _ = hamilton_blocks.shape
    slabs = lax.axis_size("slab")
    layers = lax.axis_size("layer")
    cores = 2 if layers % 2 == 0 else 1
    groups = layers // cores
    pair_count = pair_ids.shape[1]
    nb = block_order(pair_count)
    order = nb * bs
    wide = min(2 * bs, order)

    def send(value, slab_step, group_step, core_step):
        pairs = []
        for s in range(slabs):
            for g in range(groups):
                for c in range(cores):
                    there = ((s + slab_step) % slabs * groups + (g + group_step) % groups) * cores
                    pairs.append(((s * groups + g) * cores + c, there + (c + core_step) % cores))
        return lax.ppermute(value, AXES, pairs)

    table = []
    for g in range(groups):
        for s in (1, 0, -1):
            table.append(hamilton_blocks if (s, g) == (0, 0) else send(hamilton_blocks, s, g, 0))
    ids = [pair_ids] + [send(pair_ids, 0, g, 0) for g in range(1, groups)]
    scales = [weights] + [send(weights, 0, g, 0) for g in range(1, groups)]
    near, ids, scales = lax.optimization_barrier((jnp.concatenate(table), ids, scales))
    far = send(near, 0, 0, 1) if cores > 1 else near
    sizes = (slabs, groups, cores, pieces, groups, nb, bs)
    smem = pl.BlockSpec(memory_space=pltpu.SMEM)
    vmem = pl.BlockSpec(memory_space=pltpu.VMEM)
    f32, bf16 = jnp.float32, jnp.bfloat16
    square = lambda dtype: pltpu.VMEM((order, order), dtype)
    slots = 3 * pieces
    *kept, sent = pl.pallas_call(
        functools.partial(step_kernel, sizes),
        out_shape=[jax.ShapeDtypeStruct((2, pieces, bs, bs), f32)] * 3
        + [jax.ShapeDtypeStruct((2, slots, bs, bs), bf16)],
        in_specs=[smem] * (2 * groups + 1) + [vmem, vmem],
        out_specs=[vmem] * 4,
        scratch_shapes=[
            square(bf16),
            pltpu.VMEM((order // wide, wide, wide), bf16),
            pltpu.VMEM((nb, bs, bs), bf16),
            pltpu.VMEM((nb, bs, bs), bf16),
            square(bf16), square(bf16), square(bf16), square(bf16),
            square(f32), square(f32),
        ] * groups,
        compiler_params=pltpu.CompilerParams(vmem_limit_bytes=24 * 2**20),
        name="submatrix_step",
    )(*ids, *scales, potential, near, far)
    if cores > 1:
        other = send(sent, 0, 0, 1)
        kept = [
            part + other[:, i * pieces : (i + 1) * pieces].astype(f32) for i, part in enumerate(kept)
        ]
    below = send(kept[0].astype(bf16), -1, 0, 0)
    above = send(kept[2].astype(bf16), 1, 0, 0)
    totals = kept[1] + below.astype(f32) + above.astype(f32)
    return totals[0], totals[1]


def solution(mesh):
    placed = (P(AXES, None, None), P(AXES, None), P(AXES, None), P())
    return jax.shard_map(
        shards,
        mesh=mesh,
        in_specs=placed,
        out_specs=(P(AXES, None, None), P(AXES, None, None)),
        check_vma=False,
    )
```

```python
import functools

import jax
import jax.numpy as jnp
import numpy as np
from jax import lax
from jax.experimental import pallas as pl
from jax.experimental.pallas import tpu as pltpu
from jax.sharding import PartitionSpec as P

ITERS = 2
AXES = ("slab", "layer")


def block_order(pair_count):
    return (int(np.sqrt(8 * pair_count + 1)) - 1) // 2


def halves(value):
    high = value.astype(jnp.bfloat16)
    low = (value - high.astype(jnp.float32)).astype(jnp.bfloat16)
    return high, low


def mm(left, right):
    return jnp.dot(left, right, preferred_element_type=jnp.float32)


def step_kernel(sizes, *refs):
    slabs, groups, cores, pieces, rows, nb, bs = sizes
    ids, weights = refs[:rows], refs[rows : 2 * rows]
    potential, near, far, kept, sent = refs[2 * rows : 2 * rows + 5]
    scratch = refs[2 * rows + 5 :]
    per_row = len(scratch) // rows
    order = nb * bs
    wide = min(2 * bs, order)
    half_count = order // wide
    f32, bf16 = jnp.float32, jnp.bfloat16
    here_slab = lax.axis_index("slab")
    here_layer = lax.axis_index("layer")
    here_group, here_core = here_layer // cores, here_layer % cores
    mu = potential[0]
    pairs = [(a, b) for a in range(nb) for b in range(a, nb)]

    def eye(size, value):
        down = lax.broadcasted_iota(jnp.int32, (size, size), 0)
        return jnp.where(down == lax.broadcasted_iota(jnp.int32, (size, size), 1), value, 0.0)

    def strips():
        for i in range(half_count):
            for row in range(rows):
                yield i, row, pl.ds(i * wide, wide), pl.ds(i * wide, order - i * wide)

    def store_halves(high, low, upper, right, value):
        high[upper, right], low[upper, right] = halves(value)
        for j in range(right.start + wide, order, wide):
            part = pl.ds(j, wide)
            high[part, upper] = high[upper, part].T
            low[part, upper] = low[upper, part].T

    def eye_strip(upper, right, value):
        down = lax.broadcasted_iota(jnp.int32, (wide, right.size), 0)
        return jnp.where(down == lax.broadcasted_iota(jnp.int32, (wide, right.size), 1), value, 0.0)

    def where_is(row, k):
        slot_id = ids[row][0, k]
        slot = slot_id % pieces
        device = slot_id // pieces
        layer = device % (groups * cores)
        offset = (device // (groups * cores) - here_slab + 1 + slabs) % slabs
        return offset, layer // cores, layer % cores, slot

    def cut(index):
        return pl.ds(index * bs, bs)

    def low_cut(index):
        part = index * bs % wide
        return index * bs // wide, pl.ds(part, bs), pl.ds(part, bs)

    spots = [[where_is(row, k) for k in range(len(pairs))] for row in range(rows)]
    state = [scratch[row * per_row : (row + 1) * per_row] for row in range(rows)]
    inverses = []

    for row in range(rows):
        base_hi, base_lo, diag_hi, diag_lo = state[row][:4]
        base_lo[...] = jnp.zeros_like(base_lo)
        squares = jnp.zeros((bs, bs), f32)
        for k, (a, b) in enumerate(pairs):
            offset, group, core, slot = spots[row][k]
            turn = (here_group - group + groups) % groups
            index = (turn * 3 + offset) * pieces + slot
            block = near[index]
            if cores > 1:
                block = jnp.where(core == here_core, block, far[index])
            wide_block = block.astype(f32)
            if a == b:
                ham = wide_block + wide_block.T
                base = ham - eye(bs, mu)
                squares += base * base
                base_hi[cut(a), cut(a)], base_lo[low_cut(a)] = halves(base)
                diag_hi[a], diag_lo[a] = halves(ham)
            else:
                squares += 2.0 * (wide_block * wide_block)
                base_hi[cut(a), cut(b)] = block
                base_hi[cut(b), cut(a)] = block.T
        total = jnp.sum(squares, axis=(0, 1), keepdims=True)
        inverses.append(1.0 / (2.0 * jnp.sqrt(total / order + 1e-06)))

    kept[...] = jnp.zeros_like(kept)
    sent[...] = jnp.zeros_like(sent)

    for i, row, upper, right in strips():
        base_hi, base_lo, _, _, _, _, b_hi, b_lo, _, _ = state[row]
        square = mm(base_hi[upper, :], base_hi[:, right]) + mm(base_lo[i], base_hi[upper, right])
        square += jnp.concatenate(
            [mm(base_hi[upper, pl.ds(j * wide, wide)], base_lo[j]) for j in range(i, half_count)],
            axis=1,
        )
        scale = 0.5 * inverses[row] * inverses[row]
        store_halves(b_hi, b_lo, upper, right, eye_strip(upper, right, 1.5) - scale * square)
    for i, row, upper, right in strips():
        base_hi, base_lo, _, _, a_hi, a_lo, b_hi, b_lo, _, _ = state[row]
        value = mm(base_hi[upper, :], b_hi[:, right]) + mm(base_hi[upper, :], b_lo[:, right])
        value += mm(base_lo[i], b_hi[upper, right])
        store_halves(a_hi, a_lo, upper, right, -inverses[row] * value)
    for row in range(rows):
        base_hi, base_lo, diag_hi, diag_lo = state[row][:4]
        for a in range(nb):
            base_hi[cut(a), cut(a)] = diag_hi[a]
            base_lo[low_cut(a)] = diag_lo[a]
    for step in range(1, ITERS):
        for i, row, upper, right in strips():
            _, _, _, _, a_hi, a_lo, b_hi, b_lo, _, _ = state[row]
            square = mm(a_hi[upper, :], a_hi[:, right]) + mm(a_hi[upper, :], a_lo[:, right])
            square += mm(a_lo[upper, :], a_hi[:, right])
            store_halves(b_hi, b_lo, upper, right, eye_strip(upper, right, 1.5) - 0.5 * square)
        for i, row, upper, right in strips():
            _, _, _, _, a_hi, a_lo, b_hi, b_lo, full, _ = state[row]
            value = mm(a_hi[upper, :], b_hi[:, right]) + mm(a_hi[upper, :], b_lo[:, right])
            value += mm(a_lo[upper, :], b_hi[:, right])
            if step == ITERS - 1:
                value = 0.5 * (eye_strip(upper, right, 1.0) + value)
            full[upper, right] = value
        for i, row, upper, right in strips():
            _, _, _, _, a_hi, a_lo, _, _, full, _ = state[row]
            store_halves(a_hi, a_lo, upper, right, full[upper, right])
    for i, row, upper, right in strips():
        base_hi, base_lo, _, _, a_hi, a_lo, _, _, _, full2 = state[row]
        value = mm(a_hi[upper, :], base_hi[:, right]) + mm(a_lo[upper, :], base_hi[:, right])
        value += jnp.concatenate(
            [mm(a_hi[upper, pl.ds(j * wide, wide)], base_lo[j]) for j in range(i, half_count)],
            axis=1,
        )
        full2[upper, right] = value
    for row in range(rows):
        full, full2 = state[row][8:]
        for k, (a, b) in enumerate(pairs):
            offset, group, core, slot = spots[row][k]
            weight = weights[row][0, k]

            def add(target):
                at = offset * pieces + slot
                for mat, source in ((0, full), (1, full2)):
                    part = (weight * source[cut(a), cut(b)]).astype(bf16).astype(f32)
                    target[mat, at] = (target[mat, at].astype(f32) + part).astype(target.dtype)

            @pl.when(jnp.logical_and(group == here_group, core == here_core))
            def _():
                add(kept)

            if cores > 1:

                @pl.when(jnp.logical_and(group == here_group, core != here_core))
                def _():
                    add(sent)


def shards(hamilton_blocks, pair_ids, weights, potential):
    pieces, bs, _ = hamilton_blocks.shape
    slabs = lax.axis_size("slab")
    layers = lax.axis_size("layer")
    cores = 2 if layers % 2 == 0 else 1
    groups = layers // cores
    pair_count = pair_ids.shape[1]
    nb = block_order(pair_count)
    order = nb * bs
    wide = min(2 * bs, order)

    def send(value, slab_step, group_step, core_step):
        pairs = []
        for s in range(slabs):
            for g in range(groups):
                for c in range(cores):
                    there = ((s + slab_step) % slabs * groups + (g + group_step) % groups) * cores
                    pairs.append(((s * groups + g) * cores + c, there + (c + core_step) % cores))
        return lax.ppermute(value, AXES, pairs)

    table = []
    for g in range(groups):
        for s in (1, 0, -1):
            table.append(hamilton_blocks if (s, g) == (0, 0) else send(hamilton_blocks, s, g, 0))
    ids = [pair_ids] + [send(pair_ids, 0, g, 0) for g in range(1, groups)]
    scales = [weights] + [send(weights, 0, g, 0) for g in range(1, groups)]
    near, ids, scales = lax.optimization_barrier((jnp.concatenate(table), ids, scales))
    far = send(near, 0, 0, 1) if cores > 1 else near
    sizes = (slabs, groups, cores, pieces, groups, nb, bs)
    smem = pl.BlockSpec(memory_space=pltpu.SMEM)
    vmem = pl.BlockSpec(memory_space=pltpu.VMEM)
    f32, bf16 = jnp.float32, jnp.bfloat16
    square = lambda dtype: pltpu.VMEM((order, order), dtype)
    slots = 3 * pieces
    kept, sent = pl.pallas_call(
        functools.partial(step_kernel, sizes),
        out_shape=(
            jax.ShapeDtypeStruct((2, slots, bs, bs), f32),
            jax.ShapeDtypeStruct((2, slots, bs, bs), bf16),
        ),
        in_specs=[smem] * (2 * groups + 1) + [vmem, vmem],
        out_specs=(vmem, vmem),
        scratch_shapes=[
            square(bf16),
            pltpu.VMEM((order // wide, wide, wide), bf16),
            pltpu.VMEM((nb, bs, bs), bf16),
            pltpu.VMEM((nb, bs, bs), bf16),
            square(bf16), square(bf16), square(bf16), square(bf16),
            square(f32), square(f32),
        ] * groups,
        compiler_params=pltpu.CompilerParams(vmem_limit_bytes=24 * 2**20),
        name="submatrix_step",
    )(*ids, *scales, potential, near, far)
    kept = [kept[:, i * pieces : (i + 1) * pieces] for i in range(3)]
    if cores > 1:
        other = send(sent, 0, 0, 1)
        kept = [
            part + other[:, i * pieces : (i + 1) * pieces].astype(f32) for i, part in enumerate(kept)
        ]
    below = send(kept[0].astype(bf16), -1, 0, 0)
    above = send(kept[2].astype(bf16), 1, 0, 0)
    return tuple(kept[1][i] + below[i].astype(f32) + above[i].astype(f32) for i in range(2))


def solution(mesh):
    placed = (P(AXES, None, None), P(AXES, None), P(AXES, None), P())
    return jax.shard_map(
        shards,
        mesh=mesh,
        in_specs=placed,
        out_specs=(P(AXES, None, None), P(AXES, None, None)),
        check_vma=False,
    )
```

```python
import functools

import jax
import jax.numpy as jnp
import numpy as np
from jax import lax
from jax.experimental import pallas as pl
from jax.experimental.pallas import tpu as pltpu
from jax.sharding import PartitionSpec as P


ITERS = 2
AXES = ("slab", "layer")


def block_order(pair_count):
    return (int(np.sqrt(8 * pair_count + 1)) - 1) // 2


def halves(value):
    high = value.astype(jnp.bfloat16)
    low = (value - high.astype(jnp.float32)).astype(jnp.bfloat16)
    return high, low


def mm(left, right):
    return jnp.dot(left, right, preferred_element_type=jnp.float32)


def step_kernel(sizes, *refs):
    slabs, groups, cores, pieces, rows, nb, bs = sizes
    ids, weights = refs[:rows], refs[rows : 2 * rows]
    potential, near, far, kept, sent = refs[2 * rows : 2 * rows + 5]
    scratch = refs[2 * rows + 5 :]
    per_row = len(scratch) // rows
    order = nb * bs
    wide = min(2 * bs, order)
    half_count = order // wide
    f32, bf16 = jnp.float32, jnp.bfloat16
    here_slab = lax.axis_index("slab")
    here_layer = lax.axis_index("layer")
    here_group, here_core = here_layer // cores, here_layer % cores
    mu = potential[0]
    pairs = [(a, b) for a in range(nb) for b in range(a, nb)]

    def eye(size, value):
        down = lax.broadcasted_iota(jnp.int32, (size, size), 0)
        return jnp.where(down == lax.broadcasted_iota(jnp.int32, (size, size), 1), value, 0.0)

    def strips():
        for i in range(half_count):
            for row in range(rows):
                yield i, row, pl.ds(i * wide, wide), pl.ds(i * wide, order - i * wide)

    def store_halves(high, low, upper, right, value):
        high[upper, right], low[upper, right] = halves(value)
        for j in range(right.start + wide, order, wide):
            part = pl.ds(j, wide)
            high[part, upper] = high[upper, part].T
            low[part, upper] = low[upper, part].T

    def eye_strip(right, value):
        down = lax.broadcasted_iota(jnp.int32, (wide, right.size), 0)
        return jnp.where(down == lax.broadcasted_iota(jnp.int32, (wide, right.size), 1), value, 0.0)

    def where_is(row, k):
        slot_id = ids[row][0, k]
        slot = slot_id % pieces
        device = slot_id // pieces
        layer = device % (groups * cores)
        offset = (device // (groups * cores) - here_slab + 1 + slabs) % slabs
        return offset, layer // cores, layer % cores, slot

    def cut(index):
        return pl.ds(index * bs, bs)

    def low_cut(index):
        part = index * bs % wide
        return index * bs // wide, pl.ds(part, bs), pl.ds(part, bs)

    spots = [[where_is(row, k) for k in range(len(pairs))] for row in range(rows)]
    state = [scratch[row * per_row : (row + 1) * per_row] for row in range(rows)]
    inverses = []

    for row in range(rows):
        base_hi, base_lo, diag_hi, diag_lo = state[row][:4]
        base_lo[...] = jnp.zeros_like(base_lo)
        squares = jnp.zeros((bs, bs), f32)
        for k, (a, b) in enumerate(pairs):
            offset, group, core, slot = spots[row][k]
            turn = (here_group - group + groups) % groups
            place = jnp.where(here_slab % 2 == 0, offset, 2 - offset)
            index = (turn * 3 + place) * pieces + slot
            block = near[index]
            if cores > 1:
                block = jnp.where(core == here_core, block, far[index])
            wide_block = block.astype(f32)
            if a == b:
                ham = wide_block + wide_block.T
                base = ham - eye(bs, mu)
                squares += base * base
                base_hi[cut(a), cut(a)], base_lo[low_cut(a)] = halves(base)
                diag_hi[a], diag_lo[a] = halves(ham)
            else:
                squares += 2.0 * (wide_block * wide_block)
                base_hi[cut(a), cut(b)] = block
                base_hi[cut(b), cut(a)] = block.T
        total = jnp.sum(squares, axis=(0, 1), keepdims=True)
        inverses.append(1.0 / (2.0 * jnp.sqrt(total / order + 1e-06)))

    for target in (kept, sent):
        target[...] = jnp.zeros_like(target)

    for i, row, upper, right in strips():
        base_hi, base_lo, _, _, _, _, b_hi, b_lo, _, _ = state[row]
        square = mm(base_hi[upper, :], base_hi[:, right]) + mm(base_lo[i], base_hi[upper, right])
        square += jnp.concatenate(
            [mm(base_hi[upper, pl.ds(j * wide, wide)], base_lo[j]) for j in range(i, half_count)],
            axis=1,
        )
        scale = 0.5 * inverses[row] * inverses[row]
        store_halves(b_hi, b_lo, upper, right, eye_strip(right, 1.5) - scale * square)
    for i, row, upper, right in strips():
        base_hi, base_lo, _, _, a_hi, a_lo, b_hi, b_lo, _, _ = state[row]
        value = mm(base_hi[upper, :], b_hi[:, right]) + mm(base_hi[upper, :], b_lo[:, right])
        value += mm(base_lo[i], b_hi[upper, right])
        store_halves(a_hi, a_lo, upper, right, -inverses[row] * value)
    for row in range(rows):
        base_hi, base_lo, diag_hi, diag_lo = state[row][:4]
        for a in range(nb):
            base_hi[cut(a), cut(a)] = diag_hi[a]
            base_lo[low_cut(a)] = diag_lo[a]
    for step in range(1, ITERS):
        for i, row, upper, right in strips():
            _, _, _, _, a_hi, a_lo, b_hi, b_lo, _, _ = state[row]
            square = mm(a_hi[upper, :], a_hi[:, right]) + mm(a_hi[upper, :], a_lo[:, right])
            square += mm(a_lo[upper, :], a_hi[:, right])
            store_halves(b_hi, b_lo, upper, right, eye_strip(right, 1.5) - 0.5 * square)
        for i, row, upper, right in strips():
            _, _, _, _, a_hi, a_lo, b_hi, b_lo, full, _ = state[row]
            value = mm(a_hi[upper, :], b_hi[:, right]) + mm(a_hi[upper, :], b_lo[:, right])
            value += mm(a_lo[upper, :], b_hi[:, right])
            if step == ITERS - 1:
                value = 0.5 * (eye_strip(right, 1.0) + value)
            full[upper, right] = value
        for i, row, upper, right in strips():
            _, _, _, _, a_hi, a_lo, _, _, full, _ = state[row]
            store_halves(a_hi, a_lo, upper, right, full[upper, right])
    for i, row, upper, right in strips():
        base_hi, base_lo, _, _, a_hi, a_lo, _, _, _, full2 = state[row]
        value = mm(a_hi[upper, :], base_hi[:, right]) + mm(a_lo[upper, :], base_hi[:, right])
        value += jnp.concatenate(
            [mm(a_hi[upper, pl.ds(j * wide, wide)], base_lo[j]) for j in range(i, half_count)],
            axis=1,
        )
        full2[upper, right] = value
    for row in range(rows):
        full, full2 = state[row][8:]
        for k, (a, b) in enumerate(pairs):
            offset, group, core, slot = spots[row][k]
            weight = weights[row][0, k]

            def add(target):
                at = offset * pieces + slot
                for mat, source in ((0, full), (1, full2)):
                    part = (weight * source[cut(a), cut(b)]).astype(bf16).astype(f32)
                    target[mat, at] = (target[mat, at].astype(f32) + part).astype(target.dtype)

            @pl.when(jnp.logical_and(group == here_group, core == here_core))
            def _():
                add(kept)

            if cores > 1:

                @pl.when(jnp.logical_and(group == here_group, core != here_core))
                def _():
                    add(sent)


def shards(hamilton_blocks, pair_ids, weights, potential):
    pieces, bs, _ = hamilton_blocks.shape
    slabs = lax.axis_size("slab")
    layers = lax.axis_size("layer")
    cores = 2 if layers % 2 == 0 else 1
    groups = layers // cores
    pair_count = pair_ids.shape[1]
    nb = block_order(pair_count)
    order = nb * bs
    wide = min(2 * bs, order)

    def send(value, slab_of, group_step=0, core_step=0):
        pairs = []
        for s in range(slabs):
            for g in range(groups):
                for c in range(cores):
                    there = (slab_of(s) % slabs * groups + (g + group_step) % groups) * cores
                    pairs.append(((s * groups + g) * cores + c, there + (c + core_step) % cores))
        return lax.ppermute(value, AXES, pairs)

    same = lambda s: s
    first = lambda s: s - 1 if s % 2 else s + 1
    second = lambda s: s + 1 if s % 2 else s - 1
    table = [send(hamilton_blocks, second), hamilton_blocks, send(hamilton_blocks, first)]
    for g in range(1, groups):
        table += [
            send(table[0], same, g), send(hamilton_blocks, same, g), send(hamilton_blocks, first, g)
        ]
    ids = [pair_ids] + [send(pair_ids, same, g) for g in range(1, groups)]
    scales = [weights] + [send(weights, same, g) for g in range(1, groups)]
    near, ids, scales = lax.optimization_barrier((jnp.concatenate(table), ids, scales))
    far = send(near, same, 0, 1) if cores > 1 else near

    sizes = (slabs, groups, cores, pieces, groups, nb, bs)
    smem = pl.BlockSpec(memory_space=pltpu.SMEM)
    vmem = pl.BlockSpec(memory_space=pltpu.VMEM)
    f32, bf16 = jnp.float32, jnp.bfloat16
    square = lambda dtype: pltpu.VMEM((order, order), dtype)
    slots = 3 * pieces
    kept, sent = pl.pallas_call(
        functools.partial(step_kernel, sizes),
        out_shape=(
            jax.ShapeDtypeStruct((2, slots, bs, bs), f32),
            jax.ShapeDtypeStruct((2, slots, bs, bs), bf16),
        ),
        in_specs=[smem] * (2 * groups + 1) + [vmem, vmem],
        out_specs=(vmem, vmem),
        scratch_shapes=[
            square(bf16),
            pltpu.VMEM((order // wide, wide, wide), bf16),
            pltpu.VMEM((nb, bs, bs), bf16),
            pltpu.VMEM((nb, bs, bs), bf16),
            square(bf16), square(bf16), square(bf16), square(bf16),
            square(f32), square(f32),
        ] * groups,
        compiler_params=pltpu.CompilerParams(vmem_limit_bytes=24 * 2**20),
        name="submatrix_step",
    )(*ids, *scales, potential, near, far)
    kept = [kept[:, i * pieces : (i + 1) * pieces] for i in range(3)]
    if cores > 1:
        other = send(sent, same, 0, 1)
        kept = [
            part + other[:, i * pieces : (i + 1) * pieces].astype(f32) for i, part in enumerate(kept)
        ]
    below = send(kept[0].astype(bf16), lambda s: s - 1)
    above = send(kept[2].astype(bf16), lambda s: s + 1)
    return tuple(kept[1][i] + below[i].astype(f32) + above[i].astype(f32) for i in range(2))


def solution(mesh):
    placed = (P(AXES, None, None), P(AXES, None), P(AXES, None), P())

    return jax.shard_map(
        shards,
        mesh=mesh,
        in_specs=placed,
        out_specs=(P(AXES, None, None), P(AXES, None, None)),
        check_vma=False,
    )
```

```python
import functools

import jax
import jax.numpy as jnp
import numpy as np
from jax import lax
from jax.experimental import pallas as pl
from jax.experimental.pallas import tpu as pltpu
from jax.sharding import PartitionSpec as P


ITERS = 2
AXES = ("slab", "layer")


def block_order(pair_count):
    return (int(np.sqrt(8 * pair_count + 1)) - 1) // 2


def halves(value):
    high = value.astype(jnp.bfloat16)
    low = (value - high.astype(jnp.float32)).astype(jnp.bfloat16)
    return high, low


def mm(left, right):
    return jnp.dot(left, right, preferred_element_type=jnp.float32)


def step_kernel(sizes, *refs):
    slabs, groups, cores, pieces, rows, nb, bs = sizes
    ids, weights = refs[:rows], refs[rows : 2 * rows]
    potential, refs = refs[2 * rows], refs[2 * rows + 1 :]
    sources, refs = refs[: 2 * cores], refs[2 * cores :]
    kept, sent, table, scratch = refs[0], refs[1], refs[2], refs[3:]
    per_row = len(scratch) // rows
    order = nb * bs
    wide = min(2 * bs, order)
    half_count = order // wide
    f32, bf16 = jnp.float32, jnp.bfloat16
    here_slab = lax.axis_index("slab")
    here_layer = lax.axis_index("layer")
    here_group, here_core = here_layer // cores, here_layer % cores
    mu = potential[0]
    pairs = [(a, b) for a in range(nb) for b in range(a, nb)]

    def eye(size, value):
        down = lax.broadcasted_iota(jnp.int32, (size, size), 0)
        return jnp.where(down == lax.broadcasted_iota(jnp.int32, (size, size), 1), value, 0.0)

    def strips():
        for i in range(half_count):
            for row in range(rows):
                yield i, row, pl.ds(i * wide, wide), pl.ds(i * wide, order - i * wide)

    def store_halves(high, low, upper, right, value):
        high[upper, right], low[upper, right] = halves(value)
        for j in range(right.start + wide, order, wide):
            part = pl.ds(j, wide)
            high[part, upper] = high[upper, part].T
            low[part, upper] = low[upper, part].T

    def eye_strip(right, value):
        down = lax.broadcasted_iota(jnp.int32, (wide, right.size), 0)
        return jnp.where(down == lax.broadcasted_iota(jnp.int32, (wide, right.size), 1), value, 0.0)

    def where_is(row, k):
        slot_id = ids[row][0, k]
        slot = slot_id % pieces
        device = slot_id // pieces
        layer = device % (groups * cores)
        offset = (device // (groups * cores) - here_slab + 1 + slabs) % slabs
        return offset, layer // cores, layer % cores, slot

    def cut(index):
        return pl.ds(index * bs, bs)

    def low_cut(index):
        part = index * bs % wide
        return index * bs // wide, pl.ds(part, bs), pl.ds(part, bs)

    at = 0
    for source in sources:
        count = source.shape[0]
        table[pl.ds(at, count)] = source[...]
        at += count

    spots = [[where_is(row, k) for k in range(len(pairs))] for row in range(rows)]
    state = [scratch[row * per_row : (row + 1) * per_row] for row in range(rows)]
    inverses = []

    for row in range(rows):
        base_hi, base_lo, diag_hi, diag_lo = state[row][:4]
        base_lo[...] = jnp.zeros_like(base_lo)
        squares = jnp.zeros((bs, bs), f32)
        for k, (a, b) in enumerate(pairs):
            offset, group, core, slot = spots[row][k]
            turn = (here_group - group + groups) % groups
            place = jnp.where(here_slab % 2 == 0, offset, 2 - offset)
            piece = jnp.where(
                place == 1,
                jnp.where(turn == 0, 0, 1 + turn),
                jnp.where(
                    place == 2,
                    jnp.where(turn == 0, 1, groups + 1 + turn),
                    jnp.where(turn == 0, groups + 1, 2 * groups + turn),
                ),
            )
            piece += jnp.where(core == here_core, 0, 3 * groups)
            block = table[piece * pieces + slot]
            wide_block = block.astype(f32)
            if a == b:
                ham = wide_block + wide_block.T
                base = ham - eye(bs, mu)
                squares += base * base
                base_hi[cut(a), cut(a)], base_lo[low_cut(a)] = halves(base)
                diag_hi[a], diag_lo[a] = halves(ham)
            else:
                squares += 2.0 * (wide_block * wide_block)
                base_hi[cut(a), cut(b)] = block
                base_hi[cut(b), cut(a)] = block.T
        total = jnp.sum(squares, axis=(0, 1), keepdims=True)
        inverses.append(1.0 / (2.0 * jnp.sqrt(total / order + 1e-06)))

    for target in (kept, sent):
        target[...] = jnp.zeros_like(target)

    for i, row, upper, right in strips():
        base_hi, base_lo, _, _, _, _, b_hi, b_lo, _, _ = state[row]
        square = mm(base_hi[upper, :], base_hi[:, right]) + mm(base_lo[i], base_hi[upper, right])
        square += jnp.concatenate(
            [mm(base_hi[upper, pl.ds(j * wide, wide)], base_lo[j]) for j in range(i, half_count)],
            axis=1,
        )
        scale = 0.5 * inverses[row] * inverses[row]
        store_halves(b_hi, b_lo, upper, right, eye_strip(right, 1.5) - scale * square)
    for i, row, upper, right in strips():
        base_hi, base_lo, _, _, a_hi, a_lo, b_hi, b_lo, _, _ = state[row]
        value = mm(base_hi[upper, :], b_hi[:, right]) + mm(base_hi[upper, :], b_lo[:, right])
        value += mm(base_lo[i], b_hi[upper, right])
        store_halves(a_hi, a_lo, upper, right, -inverses[row] * value)
    for row in range(rows):
        base_hi, base_lo, diag_hi, diag_lo = state[row][:4]
        for a in range(nb):
            base_hi[cut(a), cut(a)] = diag_hi[a]
            base_lo[low_cut(a)] = diag_lo[a]
    for step in range(1, ITERS):
        for i, row, upper, right in strips():
            _, _, _, _, a_hi, a_lo, b_hi, b_lo, _, _ = state[row]
            square = mm(a_hi[upper, :], a_hi[:, right]) + mm(a_hi[upper, :], a_lo[:, right])
            square += mm(a_lo[upper, :], a_hi[:, right])
            store_halves(b_hi, b_lo, upper, right, eye_strip(right, 1.5) - 0.5 * square)
        for i, row, upper, right in strips():
            _, _, _, _, a_hi, a_lo, b_hi, b_lo, full, _ = state[row]
            value = mm(a_hi[upper, :], b_hi[:, right]) + mm(a_hi[upper, :], b_lo[:, right])
            value += mm(a_lo[upper, :], b_hi[:, right])
            if step == ITERS - 1:
                value = 0.5 * (eye_strip(right, 1.0) + value)
            full[upper, right] = value
        for i, row, upper, right in strips():
            _, _, _, _, a_hi, a_lo, _, _, full, _ = state[row]
            store_halves(a_hi, a_lo, upper, right, full[upper, right])
    for i, row, upper, right in strips():
        base_hi, base_lo, _, _, a_hi, a_lo, _, _, _, full2 = state[row]
        value = mm(a_hi[upper, :], base_hi[:, right]) + mm(a_lo[upper, :], base_hi[:, right])
        value += jnp.concatenate(
            [mm(a_hi[upper, pl.ds(j * wide, wide)], base_lo[j]) for j in range(i, half_count)],
            axis=1,
        )
        full2[upper, right] = value
    for row in range(rows):
        full, full2 = state[row][8:]
        for k, (a, b) in enumerate(pairs):
            offset, group, core, slot = spots[row][k]
            weight = weights[row][0, k]

            def add(target):
                at = offset * pieces + slot
                for mat, source in ((0, full), (1, full2)):
                    part = (weight * source[cut(a), cut(b)]).astype(bf16).astype(f32)
                    target[mat, at] = (target[mat, at].astype(f32) + part).astype(target.dtype)

            @pl.when(jnp.logical_and(group == here_group, core == here_core))
            def _():
                add(kept)

            if cores > 1:

                @pl.when(jnp.logical_and(group == here_group, core != here_core))
                def _():
                    add(sent)


def shards(hamilton_blocks, pair_ids, weights, potential):
    pieces, bs, _ = hamilton_blocks.shape
    slabs = lax.axis_size("slab")
    layers = lax.axis_size("layer")
    cores = 2 if layers % 2 == 0 else 1
    groups = layers // cores
    pair_count = pair_ids.shape[1]
    nb = block_order(pair_count)
    order = nb * bs
    wide = min(2 * bs, order)

    def send(value, slab_of, group_step=0, core_step=0):
        pairs = []
        for s in range(slabs):
            for g in range(groups):
                for c in range(cores):
                    there = (slab_of(s) % slabs * groups + (g + group_step) % groups) * cores
                    pairs.append(((s * groups + g) * cores + c, there + (c + core_step) % cores))
        return lax.ppermute(value, AXES, pairs)

    same = lambda s: s
    first = lambda s: s - 1 if s % 2 else s + 1
    second = lambda s: s + 1 if s % 2 else s - 1
    far_slab = send(hamilton_blocks, second)
    near = [hamilton_blocks, send(hamilton_blocks, first)]
    near += [send(hamilton_blocks, same, g) for g in range(1, groups)]
    late = [far_slab]
    late += [send(hamilton_blocks, first, g) for g in range(1, groups)]
    late += [send(far_slab, same, g) for g in range(1, groups)]
    near.append(jnp.concatenate(late))
    ids = [pair_ids] + [send(pair_ids, same, g) for g in range(1, groups)]
    scales = [weights] + [send(weights, same, g) for g in range(1, groups)]
    near = [jnp.concatenate(near[:-1]), near[-1]]
    blocks = near
    if cores > 1:
        early = send(near[0], same, 0, 1)
        near, ids, scales = lax.optimization_barrier((near, ids, scales))
        blocks = near + [early, send(near[1], same, 0, 1)]

    sizes = (slabs, groups, cores, pieces, groups, nb, bs)
    smem = pl.BlockSpec(memory_space=pltpu.SMEM)
    vmem = pl.BlockSpec(memory_space=pltpu.VMEM)
    f32, bf16 = jnp.float32, jnp.bfloat16
    square = lambda dtype: pltpu.VMEM((order, order), dtype)
    slots = 3 * pieces
    kept, sent = pl.pallas_call(
        functools.partial(step_kernel, sizes),
        out_shape=(
            jax.ShapeDtypeStruct((2, slots, bs, bs), f32),
            jax.ShapeDtypeStruct((2, slots, bs, bs), bf16),
        ),
        in_specs=[smem] * (2 * groups + 1) + [vmem] * len(blocks),
        out_specs=(vmem, vmem),
        scratch_shapes=[pltpu.VMEM((cores * 3 * groups * pieces, bs, bs), bf16)]
        + [
            square(bf16),
            pltpu.VMEM((order // wide, wide, wide), bf16),
            pltpu.VMEM((nb, bs, bs), bf16),
            pltpu.VMEM((nb, bs, bs), bf16),
            square(bf16), square(bf16), square(bf16), square(bf16),
            square(f32), square(f32),
        ] * groups,
        compiler_params=pltpu.CompilerParams(vmem_limit_bytes=24 * 2**20),
        name="submatrix_step",
    )(*ids, *scales, potential, *blocks)
    kept = [kept[:, i * pieces : (i + 1) * pieces] for i in range(3)]
    if cores > 1:
        other = send(sent, same, 0, 1)
        kept = [
            part + other[:, i * pieces : (i + 1) * pieces].astype(f32) for i, part in enumerate(kept)
        ]
    below = send(kept[0].astype(bf16), lambda s: s - 1)
    above = send(kept[2].astype(bf16), lambda s: s + 1)
    return tuple(kept[1][i] + below[i].astype(f32) + above[i].astype(f32) for i in range(2))


def solution(mesh):
    placed = (P(AXES, None, None), P(AXES, None), P(AXES, None), P())

    return jax.shard_map(
        shards,
        mesh=mesh,
        in_specs=placed,
        out_specs=(P(AXES, None, None), P(AXES, None, None)),
        check_vma=False,
    )
```

```python
import functools

import jax
import jax.numpy as jnp
import numpy as np
from jax import lax
from jax.experimental import pallas as pl
from jax.experimental.pallas import tpu as pltpu
from jax.sharding import PartitionSpec as P


ITERS = 2
AXES = ("slab", "layer")


def block_order(pair_count):
    return (int(np.sqrt(8 * pair_count + 1)) - 1) // 2


def halves(value):
    high = value.astype(jnp.bfloat16)
    low = (value - high.astype(jnp.float32)).astype(jnp.bfloat16)
    return high, low


def mm(left, right):
    return jnp.dot(left, right, preferred_element_type=jnp.float32)


def step_kernel(sizes, *refs):
    slabs, groups, cores, pieces, rows, nb, bs = sizes
    ids, weights = refs[:rows], refs[rows : 2 * rows]
    potential, refs = refs[2 * rows], refs[2 * rows + 1 :]
    sources, refs = refs[: 3 * cores], refs[3 * cores :]
    kept, sent, table, scratch = refs[0], refs[1], refs[2], refs[3:]
    per_row = len(scratch) // rows
    order = nb * bs
    wide = min(2 * bs, order)
    half_count = order // wide
    f32, bf16 = jnp.float32, jnp.bfloat16
    here_slab = lax.axis_index("slab")
    here_layer = lax.axis_index("layer")
    here_group, here_core = here_layer // cores, here_layer % cores
    mu = potential[0]
    pairs = [(a, b) for a in range(nb) for b in range(a, nb)]

    def eye(size, value):
        down = lax.broadcasted_iota(jnp.int32, (size, size), 0)
        return jnp.where(down == lax.broadcasted_iota(jnp.int32, (size, size), 1), value, 0.0)

    def strips():
        for i in range(half_count):
            for row in range(rows):
                yield i, row, pl.ds(i * wide, wide), pl.ds(i * wide, order - i * wide)

    def store_halves(high, low, upper, right, value):
        high[upper, right], low[upper, right] = halves(value)
        for j in range(right.start + wide, order, wide):
            part = pl.ds(j, wide)
            high[part, upper] = high[upper, part].T
            low[part, upper] = low[upper, part].T

    def eye_strip(right, value):
        down = lax.broadcasted_iota(jnp.int32, (wide, right.size), 0)
        return jnp.where(down == lax.broadcasted_iota(jnp.int32, (wide, right.size), 1), value, 0.0)

    def where_is(row, k):
        slot_id = ids[row][0, k]
        slot = slot_id % pieces
        device = slot_id // pieces
        layer = device % (groups * cores)
        offset = (device // (groups * cores) - here_slab + 1 + slabs) % slabs
        return offset, layer // cores, layer % cores, slot

    def cut(index):
        return pl.ds(index * bs, bs)

    def low_cut(index):
        part = index * bs % wide
        return index * bs // wide, pl.ds(part, bs), pl.ds(part, bs)

    at = 0
    for source in sources:
        count = source.shape[0]
        table[pl.ds(at, count)] = source[...]
        at += count

    spots = [[where_is(row, k) for k in range(len(pairs))] for row in range(rows)]
    state = [scratch[row * per_row : (row + 1) * per_row] for row in range(rows)]
    inverses = []

    for row in range(rows):
        base_hi, base_lo, diag_hi, diag_lo = state[row][:4]
        base_lo[...] = jnp.zeros_like(base_lo)
        squares = jnp.zeros((bs, bs), f32)
        for k, (a, b) in enumerate(pairs):
            offset, group, core, slot = spots[row][k]
            turn = (here_group - group + groups) % groups
            place = jnp.where(here_slab % 2 == 0, offset, 2 - offset)
            piece = jnp.where(
                place == 1,
                jnp.where(turn == 0, 0, 1 + turn),
                jnp.where(
                    place == 2,
                    jnp.where(turn == 0, 1, groups + 1 + turn),
                    jnp.where(turn == 0, groups + 1, 2 * groups + turn),
                ),
            )
            piece += jnp.where(core == here_core, 0, 3 * groups)
            block = table[piece * pieces + slot]
            wide_block = block.astype(f32)
            if a == b:
                ham = wide_block + wide_block.T
                base = ham - eye(bs, mu)
                squares += base * base
                base_hi[cut(a), cut(a)], base_lo[low_cut(a)] = halves(base)
                diag_hi[a], diag_lo[a] = halves(ham)
            else:
                squares += 2.0 * (wide_block * wide_block)
                base_hi[cut(a), cut(b)] = block
                base_hi[cut(b), cut(a)] = block.T
        total = jnp.sum(squares, axis=(0, 1), keepdims=True)
        inverses.append(1.0 / (2.0 * jnp.sqrt(total / order + 1e-06)))

    for target in (kept, sent):
        target[...] = jnp.zeros_like(target)

    for i, row, upper, right in strips():
        base_hi, base_lo, _, _, _, _, b_hi, b_lo, _, _ = state[row]
        square = mm(base_hi[upper, :], base_hi[:, right]) + mm(base_lo[i], base_hi[upper, right])
        square += jnp.concatenate(
            [mm(base_hi[upper, pl.ds(j * wide, wide)], base_lo[j]) for j in range(i, half_count)],
            axis=1,
        )
        scale = 0.5 * inverses[row] * inverses[row]
        store_halves(b_hi, b_lo, upper, right, eye_strip(right, 1.5) - scale * square)
    for i, row, upper, right in strips():
        base_hi, base_lo, _, _, a_hi, a_lo, b_hi, b_lo, _, _ = state[row]
        value = mm(base_hi[upper, :], b_hi[:, right]) + mm(base_hi[upper, :], b_lo[:, right])
        value += mm(base_lo[i], b_hi[upper, right])
        store_halves(a_hi, a_lo, upper, right, -inverses[row] * value)
    for row in range(rows):
        base_hi, base_lo, diag_hi, diag_lo = state[row][:4]
        for a in range(nb):
            base_hi[cut(a), cut(a)] = diag_hi[a]
            base_lo[low_cut(a)] = diag_lo[a]
    for step in range(1, ITERS):
        for i, row, upper, right in strips():
            _, _, _, _, a_hi, a_lo, b_hi, b_lo, _, _ = state[row]
            square = mm(a_hi[upper, :], a_hi[:, right]) + mm(a_hi[upper, :], a_lo[:, right])
            square += mm(a_lo[upper, :], a_hi[:, right])
            store_halves(b_hi, b_lo, upper, right, eye_strip(right, 1.5) - 0.5 * square)
        for i, row, upper, right in strips():
            _, _, _, _, a_hi, a_lo, b_hi, b_lo, full, _ = state[row]
            value = mm(a_hi[upper, :], b_hi[:, right]) + mm(a_hi[upper, :], b_lo[:, right])
            value += mm(a_lo[upper, :], b_hi[:, right])
            if step == ITERS - 1:
                value = 0.5 * (eye_strip(right, 1.0) + value)
            full[upper, right] = value
        for i, row, upper, right in strips():
            _, _, _, _, a_hi, a_lo, _, _, full, _ = state[row]
            store_halves(a_hi, a_lo, upper, right, full[upper, right])

    def parts(mat, row):
        for k, (a, b) in enumerate(pairs):
            offset, group, core, slot = spots[row][k]
            part = weights[row][0, k] * state[row][8 + mat][cut(a), cut(b)]
            same_group = group == here_group
            mine = jnp.logical_and(same_group, core == here_core)
            mates = jnp.logical_and(same_group, core != here_core)
            yield offset * pieces + slot, mine, mates, part.astype(bf16).astype(f32)

    def add(target, mat, at, part):
        target[mat, at] = (target[mat, at].astype(f32) + part).astype(target.dtype)

    for row in range(rows):
        for at, mine, mates, part in parts(0, row):
            add(kept, 0, at, jnp.where(mine, part, 0.0))
            if cores > 1:
                add(sent, 0, at, jnp.where(mates, part, 0.0))
    for i, row, upper, right in strips():
        base_hi, base_lo, _, _, a_hi, a_lo, _, _, _, full2 = state[row]
        value = mm(a_hi[upper, :], base_hi[:, right]) + mm(a_lo[upper, :], base_hi[:, right])
        value += jnp.concatenate(
            [mm(a_hi[upper, pl.ds(j * wide, wide)], base_lo[j]) for j in range(i, half_count)],
            axis=1,
        )
        full2[upper, right] = value
    for row in range(rows):
        for at, mine, mates, part in parts(1, row):
            add(kept, 1, at, jnp.where(mine, part, 0.0))
            if cores > 1:
                add(sent, 1, at, jnp.where(mates, part, 0.0))


def shards(hamilton_blocks, pair_ids, weights, potential):
    pieces, bs, _ = hamilton_blocks.shape
    slabs = lax.axis_size("slab")
    layers = lax.axis_size("layer")
    cores = 2 if layers % 2 == 0 else 1
    groups = layers // cores
    pair_count = pair_ids.shape[1]
    nb = block_order(pair_count)
    order = nb * bs
    wide = min(2 * bs, order)

    def send(value, slab_of, group_step=0, core_step=0):
        pairs = []
        for s in range(slabs):
            for g in range(groups):
                for c in range(cores):
                    there = (slab_of(s) % slabs * groups + (g + group_step) % groups) * cores
                    pairs.append(((s * groups + g) * cores + c, there + (c + core_step) % cores))
        return lax.ppermute(value, AXES, pairs)

    same = lambda s: s
    first = lambda s: s - 1 if s % 2 else s + 1
    second = lambda s: s + 1 if s % 2 else s - 1
    far_slab = send(hamilton_blocks, second)
    near = [hamilton_blocks, send(hamilton_blocks, first)]
    near += [send(hamilton_blocks, same, g) for g in range(1, groups)]
    late = [far_slab]
    late += [send(hamilton_blocks, first, g) for g in range(1, groups)]
    last = [send(far_slab, same, g) for g in range(1, groups)]
    own_ids = jnp.pad(pair_ids, ((0, 0), (0, 1)))
    own_weights = jnp.pad(weights, ((0, 0), (0, 1)))
    ids = [own_ids] + [send(pair_ids, same, g) for g in range(1, groups)]
    scales = [own_weights] + [send(weights, same, g) for g in range(1, groups)]
    near = [jnp.concatenate(part) for part in (near, late, last)]
    blocks = near
    if cores > 1:
        early = [send(part, same, 0, 1) for part in near[:2]]
        near, ids, scales = lax.optimization_barrier((near, ids, scales))
        blocks = near + early + [send(near[2], same, 0, 1)]

    sizes = (slabs, groups, cores, pieces, groups, nb, bs)
    smem = pl.BlockSpec(memory_space=pltpu.SMEM)
    vmem = pl.BlockSpec(memory_space=pltpu.VMEM)
    f32, bf16 = jnp.float32, jnp.bfloat16
    square = lambda dtype: pltpu.VMEM((order, order), dtype)
    slots = 3 * pieces
    kept, sent = pl.pallas_call(
        functools.partial(step_kernel, sizes),
        out_shape=(
            jax.ShapeDtypeStruct((2, slots, bs, bs), f32),
            jax.ShapeDtypeStruct((2, slots, bs, bs), bf16),
        ),
        in_specs=[smem] * (2 * groups + 1) + [vmem] * len(blocks),
        out_specs=(vmem, vmem),
        scratch_shapes=[pltpu.VMEM((cores * 3 * groups * pieces, bs, bs), bf16)]
        + [
            square(bf16),
            pltpu.VMEM((order // wide, wide, wide), bf16),
            pltpu.VMEM((nb, bs, bs), bf16),
            pltpu.VMEM((nb, bs, bs), bf16),
            square(bf16), square(bf16), square(bf16), square(bf16),
            square(f32), square(f32),
        ] * groups,
        compiler_params=pltpu.CompilerParams(vmem_limit_bytes=24 * 2**20),
        name="submatrix_step",
    )(*ids, *scales, potential, *blocks)
    kept = [kept[:, i * pieces : (i + 1) * pieces] for i in range(3)]
    if cores > 1:
        other = send(sent, same, 0, 1)
        kept = [
            part + other[:, i * pieces : (i + 1) * pieces].astype(f32) for i, part in enumerate(kept)
        ]
    below = send(kept[0].astype(bf16), lambda s: s - 1)
    above = send(kept[2].astype(bf16), lambda s: s + 1)
    return tuple(kept[1][i] + below[i].astype(f32) + above[i].astype(f32) for i in range(2))


def solution(mesh):
    placed = (P(AXES, None, None), P(AXES, None), P(AXES, None), P())

    return jax.shard_map(
        shards,
        mesh=mesh,
        in_specs=placed,
        out_specs=(P(AXES, None, None), P(AXES, None, None)),
        check_vma=False,
    )
```

```python
import functools

import jax
import jax.numpy as jnp
import numpy as np
from jax import lax
from jax.experimental import pallas as pl
from jax.experimental.pallas import tpu as pltpu
from jax.sharding import PartitionSpec as P


ITERS = 2
AXES = ("slab", "layer")


def block_order(pair_count):
    return (int(np.sqrt(8 * pair_count + 1)) - 1) // 2


def halves(value):
    high = value.astype(jnp.bfloat16)
    low = (value - high.astype(jnp.float32)).astype(jnp.bfloat16)
    return high, low


def mm(left, right):
    return jnp.dot(left, right, preferred_element_type=jnp.float32)


def step_kernel(sizes, *refs):
    slabs, groups, cores, pieces, rows, nb, bs = sizes
    ids, weights = refs[:rows], refs[rows : 2 * rows]
    potential, refs = refs[2 * rows], refs[2 * rows + 1 :]
    sources, refs = refs[: 3 * cores], refs[3 * cores :]
    kept, sent, table, scratch = refs[0], refs[1], refs[2], refs[3:]
    per_row = len(scratch) // rows
    order = nb * bs
    wide = min(2 * bs, order)
    half_count = order // wide
    f32, bf16 = jnp.float32, jnp.bfloat16
    here_slab = lax.axis_index("slab")
    here_layer = lax.axis_index("layer")
    here_group, here_core = here_layer // cores, here_layer % cores
    mu = potential[0]
    pairs = [(a, b) for a in range(nb) for b in range(a, nb)]

    def eye(size, value):
        down = lax.broadcasted_iota(jnp.int32, (size, size), 0)
        return jnp.where(down == lax.broadcasted_iota(jnp.int32, (size, size), 1), value, 0.0)

    def strips():
        for i in range(half_count):
            for row in range(rows):
                yield i, row, pl.ds(i * wide, wide), pl.ds(i * wide, order - i * wide)

    def store_halves(high, low, upper, right, value):
        high[upper, right], low[upper, right] = halves(value)
        for j in range(right.start + wide, order, wide):
            part = pl.ds(j, wide)
            high[part, upper] = high[upper, part].T
            low[part, upper] = low[upper, part].T

    def eye_strip(right, value):
        down = lax.broadcasted_iota(jnp.int32, (wide, right.size), 0)
        return jnp.where(down == lax.broadcasted_iota(jnp.int32, (wide, right.size), 1), value, 0.0)

    def where_is(row, k):
        slot_id = ids[row][0, k]
        slot = slot_id % pieces
        device = slot_id // pieces
        layer = device % (groups * cores)
        offset = (device // (groups * cores) - here_slab + 1 + slabs) % slabs
        return offset, layer // cores, layer % cores, slot

    def cut(index):
        return pl.ds(index * bs, bs)

    def low_cut(index):
        part = index * bs % wide
        return index * bs // wide, pl.ds(part, bs), pl.ds(part, bs)

    at = 0
    for source in sources:
        count = source.shape[0]
        table[pl.ds(at, count)] = source[...]
        at += count

    spots = [[where_is(row, k) for k in range(len(pairs))] for row in range(rows)]
    state = [scratch[row * per_row : (row + 1) * per_row] for row in range(rows)]
    inverses = []

    for row in range(rows):
        base_hi, base_lo, diag_hi, diag_lo = state[row][:4]
        base_lo[...] = jnp.zeros_like(base_lo)
        squares = jnp.zeros((bs, bs), f32)
        for k, (a, b) in enumerate(pairs):
            offset, group, core, slot = spots[row][k]
            turn = (here_group - group + groups) % groups
            place = jnp.where(here_slab % 2 == 0, offset, 2 - offset)
            piece = jnp.where(
                place == 1,
                jnp.where(turn == 0, 0, 1 + turn),
                jnp.where(
                    place == 2,
                    jnp.where(turn == 0, 1, groups + 1 + turn),
                    jnp.where(turn == 0, groups + 1, 2 * groups + turn),
                ),
            )
            piece += jnp.where(core == here_core, 0, 3 * groups)
            block = table[piece * pieces + slot]
            wide_block = block.astype(f32)
            if a == b:
                ham = wide_block + wide_block.T
                base = ham - eye(bs, mu)
                squares += base * base
                base_hi[cut(a), cut(a)], base_lo[low_cut(a)] = halves(base)
                diag_hi[a], diag_lo[a] = halves(ham)
            else:
                squares += 2.0 * (wide_block * wide_block)
                base_hi[cut(a), cut(b)] = block
                base_hi[cut(b), cut(a)] = block.T
        total = jnp.sum(squares, axis=(0, 1), keepdims=True)
        inverses.append(1.0 / (2.0 * jnp.sqrt(total / order + 1e-06)))

    for target in (kept, sent):
        target[...] = jnp.zeros_like(target)

    for i, row, upper, right in strips():
        base_hi, base_lo, _, _, _, _, b_hi, b_lo, _, _ = state[row]
        square = mm(base_hi[upper, :], base_hi[:, right]) + mm(base_lo[i], base_hi[upper, right])
        square += jnp.concatenate(
            [mm(base_hi[upper, pl.ds(j * wide, wide)], base_lo[j]) for j in range(i, half_count)],
            axis=1,
        )
        scale = 0.5 * inverses[row] * inverses[row]
        store_halves(b_hi, b_lo, upper, right, eye_strip(right, 1.5) - scale * square)
    for i, row, upper, right in strips():
        base_hi, base_lo, _, _, a_hi, a_lo, b_hi, b_lo, _, _ = state[row]
        value = mm(base_hi[upper, :], b_hi[:, right]) + mm(base_hi[upper, :], b_lo[:, right])
        value += mm(base_lo[i], b_hi[upper, right])
        store_halves(a_hi, a_lo, upper, right, -inverses[row] * value)
    for row in range(rows):
        base_hi, base_lo, diag_hi, diag_lo = state[row][:4]
        for a in range(nb):
            base_hi[cut(a), cut(a)] = diag_hi[a]
            base_lo[low_cut(a)] = diag_lo[a]
    for step in range(1, ITERS):
        for i, row, upper, right in strips():
            _, _, _, _, a_hi, a_lo, b_hi, b_lo, _, _ = state[row]
            square = mm(a_hi[upper, :], a_hi[:, right]) + mm(a_hi[upper, :], a_lo[:, right])
            square += mm(a_lo[upper, :], a_hi[:, right])
            store_halves(b_hi, b_lo, upper, right, eye_strip(right, 1.5) - 0.5 * square)
        for i, row, upper, right in strips():
            _, _, _, _, a_hi, a_lo, b_hi, b_lo, full, _ = state[row]
            value = mm(a_hi[upper, :], b_hi[:, right]) + mm(a_hi[upper, :], b_lo[:, right])
            value += mm(a_lo[upper, :], b_hi[:, right])
            if step == ITERS - 1:
                value = 0.5 * (eye_strip(right, 1.0) + value)
            full[upper, right] = value
        for i, row, upper, right in strips():
            _, _, _, _, a_hi, a_lo, _, _, full, _ = state[row]
            store_halves(a_hi, a_lo, upper, right, full[upper, right])

    def parts(mat, row):
        for k, (a, b) in enumerate(pairs):
            offset, group, core, slot = spots[row][k]
            part = weights[row][0, k] * state[row][8 + mat][cut(a), cut(b)]
            same_group = group == here_group
            mine = jnp.logical_and(same_group, core == here_core)
            mates = jnp.logical_and(same_group, core != here_core)
            turned = jnp.where(offset == 1, 2, offset // 2) * pieces + slot
            yield offset * pieces + slot, turned, mine, mates, part.astype(bf16).astype(f32)

    def add(target, where, part):
        target[where] = (target[where].astype(f32) + part).astype(target.dtype)

    for row in range(rows):
        for at, turned, mine, mates, part in parts(0, row):
            add(kept, (0, at), jnp.where(mine, part, 0.0))
            if cores > 1:
                add(sent, (turned, 0), jnp.where(mates, part, 0.0))
    for i, row, upper, right in strips():
        base_hi, base_lo, _, _, a_hi, a_lo, _, _, _, full2 = state[row]
        value = mm(a_hi[upper, :], base_hi[:, right]) + mm(a_lo[upper, :], base_hi[:, right])
        value += jnp.concatenate(
            [mm(a_hi[upper, pl.ds(j * wide, wide)], base_lo[j]) for j in range(i, half_count)],
            axis=1,
        )
        full2[upper, right] = value
    for row in range(rows):
        for at, turned, mine, mates, part in parts(1, row):
            add(kept, (1, at), jnp.where(mine, part, 0.0))
            if cores > 1:
                add(sent, (turned, 1), jnp.where(mates, part, 0.0))


def shards(hamilton_blocks, pair_ids, weights, potential):
    pieces, bs, _ = hamilton_blocks.shape
    slabs = lax.axis_size("slab")
    layers = lax.axis_size("layer")
    cores = 2 if layers % 2 == 0 else 1
    groups = layers // cores
    pair_count = pair_ids.shape[1]
    nb = block_order(pair_count)
    order = nb * bs
    wide = min(2 * bs, order)

    def send(value, slab_of, group_step=0, core_step=0):
        pairs = []
        for s in range(slabs):
            for g in range(groups):
                for c in range(cores):
                    there = (slab_of(s) % slabs * groups + (g + group_step) % groups) * cores
                    pairs.append(((s * groups + g) * cores + c, there + (c + core_step) % cores))
        return lax.ppermute(value, AXES, pairs)

    same = lambda s: s
    first = lambda s: s - 1 if s % 2 else s + 1
    second = lambda s: s + 1 if s % 2 else s - 1
    far_slab = send(hamilton_blocks, second)
    near = [hamilton_blocks, send(hamilton_blocks, first)]
    near += [send(hamilton_blocks, same, g) for g in range(1, groups)]
    late = [far_slab]
    late += [send(hamilton_blocks, first, g) for g in range(1, groups)]
    last = [send(far_slab, same, g) for g in range(1, groups)]
    own_ids = jnp.pad(pair_ids, ((0, 0), (0, 1)))
    own_weights = jnp.pad(weights, ((0, 0), (0, 1)))
    ids = [own_ids] + [send(pair_ids, same, g) for g in range(1, groups)]
    scales = [own_weights] + [send(weights, same, g) for g in range(1, groups)]
    near = [jnp.concatenate(part) for part in (near, late, last)]
    blocks = near
    if cores > 1:
        early = [send(part, same, 0, 1) for part in near[:2]]
        near, ids, scales = lax.optimization_barrier((near, ids, scales))
        blocks = near + early + [send(near[2], same, 0, 1)]

    sizes = (slabs, groups, cores, pieces, groups, nb, bs)
    smem = pl.BlockSpec(memory_space=pltpu.SMEM)
    vmem = pl.BlockSpec(memory_space=pltpu.VMEM)
    f32, bf16 = jnp.float32, jnp.bfloat16
    square = lambda dtype: pltpu.VMEM((order, order), dtype)
    slots = 3 * pieces
    kept, sent = pl.pallas_call(
        functools.partial(step_kernel, sizes),
        out_shape=(
            jax.ShapeDtypeStruct((2, slots, bs, bs), f32),
            jax.ShapeDtypeStruct((slots, 2, bs, bs), bf16),
        ),
        in_specs=[smem] * (2 * groups + 1) + [vmem] * len(blocks),
        out_specs=(vmem, vmem),
        scratch_shapes=[pltpu.VMEM((cores * 3 * groups * pieces, bs, bs), bf16)]
        + [
            square(bf16),
            pltpu.VMEM((order // wide, wide, wide), bf16),
            pltpu.VMEM((nb, bs, bs), bf16),
            pltpu.VMEM((nb, bs, bs), bf16),
            square(bf16), square(bf16), square(bf16), square(bf16),
            square(f32), square(f32),
        ] * groups,
        compiler_params=pltpu.CompilerParams(vmem_limit_bytes=24 * 2**20),
        name="submatrix_step",
    )(*ids, *scales, potential, *blocks)
    kept = [kept[:, i * pieces : (i + 1) * pieces] for i in range(3)]
    if cores > 1:
        leaving = jnp.swapaxes(send(sent[: 2 * pieces], same, 0, 1), 0, 1)
        staying = send(sent[2 * pieces :], same, 0, 1)
        kept[0] += leaving[:, :pieces].astype(f32)
        kept[2] += leaving[:, pieces:].astype(f32)
    below = send(kept[0].astype(bf16), lambda s: s - 1)
    above = send(kept[2].astype(bf16), lambda s: s + 1)
    last = [below, above]
    if cores > 1:
        last = lax.optimization_barrier(last + [staying])
        last[2] = jnp.swapaxes(last[2], 0, 1)
    return tuple(kept[1][i] + sum(part[i].astype(f32) for part in last) for i in range(2))


def solution(mesh):
    placed = (P(AXES, None, None), P(AXES, None), P(AXES, None), P())

    return jax.shard_map(
        shards,
        mesh=mesh,
        in_specs=placed,
        out_specs=(P(AXES, None, None), P(AXES, None, None)),
        check_vma=False,
    )
```

```python
import functools

import jax
import jax.numpy as jnp
import numpy as np
from jax import lax
from jax.experimental import pallas as pl
from jax.experimental.pallas import tpu as pltpu
from jax.sharding import PartitionSpec as P


ITERS = 2
AXES = ("slab", "layer")


def block_order(pair_count):
    return (int(np.sqrt(8 * pair_count + 1)) - 1) // 2


def halves(value):
    high = value.astype(jnp.bfloat16)
    low = (value - high.astype(jnp.float32)).astype(jnp.bfloat16)
    return high, low


def mm(left, right):
    return jnp.dot(left, right, preferred_element_type=jnp.float32)


def step_kernel(sizes, *refs):
    slabs, groups, cores, pieces, rows, nb, bs = sizes
    ids, weights = refs[:rows], refs[rows : 2 * rows]
    potential, refs = refs[2 * rows], refs[2 * rows + 1 :]
    sources, refs = refs[: 3 * cores], refs[3 * cores :]
    kept, sent, table, scratch = refs[0], refs[1], refs[2], refs[3:]
    per_row = len(scratch) // rows
    order = nb * bs
    wide = min(2 * bs, order)
    half_count = order // wide
    f32, bf16 = jnp.float32, jnp.bfloat16
    here_slab = lax.axis_index("slab")
    here_layer = lax.axis_index("layer")
    here_group, here_core = here_layer // cores, here_layer % cores
    mu = potential[0]
    pairs = [(a, b) for a in range(nb) for b in range(a, nb)]

    def eye(size, value):
        down = lax.broadcasted_iota(jnp.int32, (size, size), 0)
        return jnp.where(down == lax.broadcasted_iota(jnp.int32, (size, size), 1), value, 0.0)

    def strips():
        for i in range(half_count):
            for row in range(rows):
                yield i, row, pl.ds(i * wide, wide), pl.ds(i * wide, order - i * wide)

    def store_halves(high, low, upper, right, value):
        high[upper, right], low[upper, right] = halves(value)
        for j in range(right.start + wide, order, wide):
            part = pl.ds(j, wide)
            high[part, upper] = high[upper, part].T
            low[part, upper] = low[upper, part].T

    def eye_strip(right, value):
        down = lax.broadcasted_iota(jnp.int32, (wide, right.size), 0)
        return jnp.where(down == lax.broadcasted_iota(jnp.int32, (wide, right.size), 1), value, 0.0)

    def where_is(row, k):
        slot_id = ids[row][0, k]
        slot = slot_id % pieces
        device = slot_id // pieces
        layer = device % (groups * cores)
        offset = (device // (groups * cores) - here_slab + 1 + slabs) % slabs
        return offset, layer // cores, layer % cores, slot

    def cut(index):
        return pl.ds(index * bs, bs)

    def low_cut(index):
        part = index * bs % wide
        return index * bs // wide, pl.ds(part, bs), pl.ds(part, bs)

    at = 0
    for source in sources:
        count = source.shape[0]
        table[pl.ds(at, count)] = source[...]
        at += count

    spots = [[where_is(row, k) for k in range(len(pairs))] for row in range(rows)]
    state = [scratch[row * per_row : (row + 1) * per_row] for row in range(rows)]
    inverses = []

    for row in range(rows):
        base_hi, base_lo, diag_hi, diag_lo = state[row][:4]
        base_lo[...] = jnp.zeros_like(base_lo)
        squares = jnp.zeros((bs, bs), f32)
        for k, (a, b) in enumerate(pairs):
            offset, group, core, slot = spots[row][k]
            turn = (here_group - group + groups) % groups
            place = jnp.where(here_slab % 2 == 0, offset, 2 - offset)
            piece = jnp.where(
                place == 1,
                jnp.where(turn == 0, 0, 1 + turn),
                jnp.where(
                    place == 2,
                    jnp.where(turn == 0, 1, groups + 1 + turn),
                    jnp.where(turn == 0, groups + 1, 2 * groups + turn),
                ),
            )
            piece += jnp.where(core == here_core, 0, 3 * groups)
            block = table[piece * pieces + slot]
            wide_block = block.astype(f32)
            if a == b:
                ham = wide_block + wide_block.T
                base = ham - eye(bs, mu)
                squares += base * base
                base_hi[cut(a), cut(a)], base_lo[low_cut(a)] = halves(base)
                diag_hi[a], diag_lo[a] = halves(ham)
            else:
                squares += 2.0 * (wide_block * wide_block)
                base_hi[cut(a), cut(b)] = block
                base_hi[cut(b), cut(a)] = block.T
        total = jnp.sum(squares, axis=(0, 1), keepdims=True)
        inverses.append(1.0 / (2.0 * jnp.sqrt(total / order + 1e-06)))

    for target in (kept, sent):
        target[...] = jnp.zeros_like(target)

    for i, row, upper, right in strips():
        base_hi, base_lo, _, _, _, _, b_hi, b_lo, _, _ = state[row]
        square = mm(base_hi[upper, :], base_hi[:, right]) + mm(base_lo[i], base_hi[upper, right])
        square += jnp.concatenate(
            [mm(base_hi[upper, pl.ds(j * wide, wide)], base_lo[j]) for j in range(i, half_count)],
            axis=1,
        )
        scale = 0.5 * inverses[row] * inverses[row]
        store_halves(b_hi, b_lo, upper, right, eye_strip(right, 1.5) - scale * square)
    for i, row, upper, right in strips():
        base_hi, base_lo, _, _, a_hi, a_lo, b_hi, b_lo, _, _ = state[row]
        value = mm(base_hi[upper, :], b_hi[:, right]) + mm(base_hi[upper, :], b_lo[:, right])
        value += mm(base_lo[i], b_hi[upper, right])
        store_halves(a_hi, a_lo, upper, right, -inverses[row] * value)
    for row in range(rows):
        base_hi, base_lo, diag_hi, diag_lo = state[row][:4]
        for a in range(nb):
            base_hi[cut(a), cut(a)] = diag_hi[a]
            base_lo[low_cut(a)] = diag_lo[a]
    for step in range(1, ITERS):
        for i, row, upper, right in strips():
            _, _, _, _, a_hi, a_lo, b_hi, b_lo, _, _ = state[row]
            square = mm(a_hi[upper, :], a_hi[:, right]) + mm(a_hi[upper, :], a_lo[:, right])
            square += mm(a_lo[upper, :], a_hi[:, right])
            store_halves(b_hi, b_lo, upper, right, eye_strip(right, 1.5) - 0.5 * square)
        for i, row, upper, right in strips():
            _, _, _, _, a_hi, a_lo, b_hi, b_lo, full, _ = state[row]
            value = mm(a_hi[upper, :], b_hi[:, right]) + mm(a_hi[upper, :], b_lo[:, right])
            value += mm(a_lo[upper, :], b_hi[:, right])
            if step == ITERS - 1:
                value = 0.5 * (eye_strip(right, 1.0) + value)
            full[upper, right] = value
        for i, row, upper, right in strips():
            _, _, _, _, a_hi, a_lo, _, _, full, _ = state[row]
            store_halves(a_hi, a_lo, upper, right, full[upper, right])

    def parts(mat, row):
        for k, (a, b) in enumerate(pairs):
            offset, group, core, slot = spots[row][k]
            part = weights[row][0, k] * state[row][8 + mat][cut(a), cut(b)]
            same_group = group == here_group
            mine = jnp.logical_and(same_group, core == here_core)
            mates = jnp.logical_and(same_group, core != here_core)
            turned = jnp.where(offset == 1, 2, offset // 2) * pieces + slot
            yield offset * pieces + slot, turned, mine, mates, part.astype(bf16).astype(f32)

    def add(target, where, part):
        target[where] = (target[where].astype(f32) + part).astype(target.dtype)

    for row in range(rows):
        for at, turned, mine, mates, part in parts(0, row):
            add(kept, (at, 0), jnp.where(mine, part, 0.0))
            if cores > 1:
                add(sent, (turned, 0), jnp.where(mates, part, 0.0))
    for i, row, upper, right in strips():
        base_hi, base_lo, _, _, a_hi, a_lo, _, _, _, full2 = state[row]
        value = mm(a_hi[upper, :], base_hi[:, right]) + mm(a_lo[upper, :], base_hi[:, right])
        value += jnp.concatenate(
            [mm(a_hi[upper, pl.ds(j * wide, wide)], base_lo[j]) for j in range(i, half_count)],
            axis=1,
        )
        full2[upper, right] = value
    for row in range(rows):
        for at, turned, mine, mates, part in parts(1, row):
            add(kept, (at, 1), jnp.where(mine, part, 0.0))
            if cores > 1:
                add(sent, (turned, 1), jnp.where(mates, part, 0.0))


def shards(hamilton_blocks, pair_ids, weights, potential):
    pieces, bs, _ = hamilton_blocks.shape
    slabs = lax.axis_size("slab")
    layers = lax.axis_size("layer")
    cores = 2 if layers % 2 == 0 else 1
    groups = layers // cores
    pair_count = pair_ids.shape[1]
    nb = block_order(pair_count)
    order = nb * bs
    wide = min(2 * bs, order)

    def send(value, slab_of, group_step=0, core_step=0):
        pairs = []
        for s in range(slabs):
            for g in range(groups):
                for c in range(cores):
                    there = (slab_of(s) % slabs * groups + (g + group_step) % groups) * cores
                    pairs.append(((s * groups + g) * cores + c, there + (c + core_step) % cores))
        return lax.ppermute(value, AXES, pairs)

    same = lambda s: s
    first = lambda s: s - 1 if s % 2 else s + 1
    second = lambda s: s + 1 if s % 2 else s - 1
    far_slab = send(hamilton_blocks, second)
    near = [hamilton_blocks, send(hamilton_blocks, first)]
    near += [send(hamilton_blocks, same, g) for g in range(1, groups)]
    late = [far_slab]
    late += [send(hamilton_blocks, first, g) for g in range(1, groups)]
    last = [send(far_slab, same, g) for g in range(1, groups)]
    own_ids = jnp.pad(pair_ids, ((0, 0), (0, 1)))
    own_weights = jnp.pad(weights, ((0, 0), (0, 1)))
    ids = [own_ids] + [send(pair_ids, same, g) for g in range(1, groups)]
    scales = [own_weights] + [send(weights, same, g) for g in range(1, groups)]
    near = [jnp.concatenate(part) for part in (near, late, last)]
    blocks = near
    if cores > 1:
        early = [send(part, same, 0, 1) for part in near[:2]]
        near, ids, scales = lax.optimization_barrier((near, ids, scales))
        blocks = near + early + [send(near[2], same, 0, 1)]

    sizes = (slabs, groups, cores, pieces, groups, nb, bs)
    smem = pl.BlockSpec(memory_space=pltpu.SMEM)
    vmem = pl.BlockSpec(memory_space=pltpu.VMEM)
    f32, bf16 = jnp.float32, jnp.bfloat16
    square = lambda dtype: pltpu.VMEM((order, order), dtype)
    slots = 3 * pieces
    kept, sent = pl.pallas_call(
        functools.partial(step_kernel, sizes),
        out_shape=(
            jax.ShapeDtypeStruct((slots, 2, bs, bs), f32),
            jax.ShapeDtypeStruct((slots, 2, bs, bs), bf16),
        ),
        in_specs=[smem] * (2 * groups + 1) + [vmem] * len(blocks),
        out_specs=(vmem, vmem),
        scratch_shapes=[pltpu.VMEM((cores * 3 * groups * pieces, bs, bs), bf16)]
        + [
            square(bf16),
            pltpu.VMEM((order // wide, wide, wide), bf16),
            pltpu.VMEM((nb, bs, bs), bf16),
            pltpu.VMEM((nb, bs, bs), bf16),
            square(bf16), square(bf16), square(bf16), square(bf16),
            square(f32), square(f32),
        ] * groups,
        compiler_params=pltpu.CompilerParams(vmem_limit_bytes=24 * 2**20),
        name="submatrix_step",
    )(*ids, *scales, potential, *blocks)
    kept = [kept[i * pieces : (i + 1) * pieces] for i in range(3)]
    mate = [sent[i * pieces : (i + 1) * pieces] for i in range(3)]
    if cores > 1:
        mate = [send(part, same, 0, 1) for part in mate]
        kept[0] = kept[0] + mate[0].astype(f32)
        kept[2] = lax.optimization_barrier(kept[2]) + mate[1].astype(f32)
    below = send(kept[0].astype(bf16), lambda s: s - 1)
    above = send(kept[2].astype(bf16), lambda s: s + 1)
    last = [below, above]
    if cores > 1:
        last = lax.optimization_barrier(last + [mate[2]])
    total = [kept[1][:, i] + sum(part[:, i].astype(f32) for part in last) for i in range(2)]
    return tuple(total)


def solution(mesh):
    placed = (P(AXES, None, None), P(AXES, None), P(AXES, None), P())

    return jax.shard_map(
        shards,
        mesh=mesh,
        in_specs=placed,
        out_specs=(P(AXES, None, None), P(AXES, None, None)),
        check_vma=False,
    )
```
